32 devices in a mesh: data: 2 (over x), store: 4 (over z), model: 4 (over y, core).
Axes of the slice: x: 2, y: 2, z: 4, core: 2. Of those that a mesh axis runs over, the one named last changes fastest.
Arguments:
- queries: bfloat16 [512, 4096], P('data'), parts along dimension 0
- w_head: bfloat16 [4096, 32000], P(None, 'model')
- store_keys: bfloat16 [131072, 4096], P(('store', 'model'))
- store_tok: int32 [131072], P(('store', 'model'))
- temperature: float32 [], replicated
- mix_weight: float32 [], replicated
Outputs:
- output: float32 [512, 32000], P(('data', 'store'), 'model'), parts along dimension 0
There are 2 independent parts. The reference program is written for one: setup_inputs(seed, part) draws one part's arguments, and reference() takes and returns one part's arrays. A program takes and returns all parts, laid end to end along the dimension named above; an argument that names none is the same for every part.
All inputs are finite; a program needn't handle non-finite values.
Results may differ from the reference program's by a relative error of at most 0.001.
Values are sent between devices in bfloat16 or wider.
A program may use at most 1 GiB of HBM per device.

```python
import jax
import jax.numpy as jnp
from jax import lax

HIDDEN = 4096
VOCAB = 32000
ROWS_DEV = 64
KEYS_DEV = 8192
STORE_DEVS = 4
MODEL_DEVS = 4
BATCH = ROWS_DEV * STORE_DEVS
SHARDS = STORE_DEVS * MODEL_DEVS
N_KEYS = KEYS_DEV * SHARDS


def setup_inputs(seed: int = 0, part: int = 0) -> dict:
    base_key = jax.random.key(seed)
    part_key = jax.random.fold_in(base_key, part)
    key_head, key_store, key_tok_a, key_tok_b, key_temp, key_mix = jax.random.split(base_key, 6)
    queries = jax.random.normal(part_key, (BATCH, HIDDEN), jnp.float32)
    w_head = jax.random.normal(key_head, (HIDDEN, VOCAB), jnp.float32) * HIDDEN ** -0.5
    store_keys = jax.random.normal(key_store, (N_KEYS, HIDDEN), jnp.float32)
    tok_a = jax.random.randint(key_tok_a, (N_KEYS,), 0, VOCAB, jnp.int32)
    tok_b = jax.random.randint(key_tok_b, (N_KEYS,), 0, VOCAB, jnp.int32)
    store_tok = jnp.minimum(tok_a, tok_b).at[0].set(0).at[N_KEYS - 1].set(VOCAB - 1)
    temperature = (6.0 * HIDDEN) ** 0.5 / 1.5 * jax.random.uniform(key_temp, (), jnp.float32, minval=0.6, maxval=1.5)
    mix_weight = jax.random.uniform(key_mix, (), jnp.float32, minval=0.25, maxval=0.5)
    return {"queries": queries.astype(jnp.bfloat16), "w_head": w_head.astype(jnp.bfloat16), "store_keys": store_keys.astype(jnp.bfloat16), "store_tok": store_tok, "temperature": temperature, "mix_weight": mix_weight}


def reference(queries, w_head, store_keys, store_tok, temperature, mix_weight):
    key_blocks = store_keys.reshape(SHARDS, KEYS_DEV, HIDDEN)
    tok_blocks = store_tok.reshape(SHARDS, KEYS_DEV)

    def block_scores(block):
        key_dots = jnp.dot(block, queries.T, preferred_element_type=jnp.float32)
        key_norms = jnp.sum(jnp.square(block.astype(jnp.float32)), axis=1)
        return (2.0 * key_dots - key_norms[:, None]) / temperature

    block_top = lax.map(lambda block: jnp.max(block_scores(block), axis=0), key_blocks)
    row_top = jnp.max(block_top, axis=0)

    def accumulate(carry, pair):
        histogram, row_total = carry
        block, tok_ids = pair
        weights = jnp.exp(block_scores(block) - row_top)
        histogram = histogram + jax.ops.segment_sum(weights, tok_ids, num_segments=VOCAB)
        row_total = row_total + jnp.sum(weights, axis=0)
        return (histogram, row_total), None

    init_state = (jnp.zeros((VOCAB, BATCH), jnp.float32), jnp.zeros((BATCH,), jnp.float32))
    (histogram, row_total), _ = lax.scan(accumulate, init_state, (key_blocks, tok_blocks))
    knn_prob = (histogram / row_total).T
    logits = jnp.dot(queries, w_head, preferred_element_type=jnp.float32)
    lm_exp = jnp.exp(logits - jnp.max(logits, axis=1, keepdims=True))
    lm_prob = lm_exp / jnp.sum(lm_exp, axis=1, keepdims=True)
    return jnp.log(mix_weight * knn_prob + (1.0 - mix_weight) * lm_prob)
```

```python
import functools

import jax
import jax.numpy as jnp
from jax import lax
from jax.experimental import pallas as pl
from jax.experimental.pallas import tpu as pltpu
from jax.sharding import PartitionSpec as P


LANES = 128
BLOCK = 512
BATCH = 16
VOCAB_LOC = 8000
PIECE = 4096
FIRST = 4
META = 8
SLOTS = 4
SCATTER_VMEM = 30 * 1024 * 1024
STEP = 976
UPPER = VOCAB_LOC - PIECE
FLAG = 1 << 16
CLASH = 1 << 17


def targets(me):
    left = me < 2
    return me, me ^ 1, jnp.where(left, 2, 1), jnp.where(left, 3, 0)


def scores_kernel(first, count, s_ref, tau_ref, q_ref, k_hbm, own_ref, near_ref, sparse_ref, dense_ref, qs_ref, held, sem):
    def fetch(block):
        slot = lax.rem(block, SLOTS)
        rows = pl.ds(pl.multiple_of((first + block) * BLOCK, BLOCK), BLOCK)
        return pltpu.make_async_copy(k_hbm.at[rows], held.at[slot], sem.at[slot])

    for block in range(SLOTS - 1):
        fetch(block).start()
    for k, z in enumerate(targets(s_ref[0])):
        qs_ref[64 * k:64 * k + 64, :] = q_ref[pl.ds(pl.multiple_of(z * 64, 64), 64), :]
    half = BLOCK // 2
    low = lax.broadcasted_iota(jnp.int32, (half, LANES), 1) < 64

    @pl.loop(0, count)
    def _(block):
        @pl.when(block + SLOTS - 1 < count)
        def _():
            fetch(block + SLOTS - 1).start()

        fetch(block).wait()
        keys = held[lax.rem(block, SLOTS)]
        dots = lax.dot_general(keys, qs_ref[...], (((1,), (1,)), ((), ())), preferred_element_type=jnp.float32)
        wide = keys.astype(jnp.float32)
        norms = jnp.sum(wide * wide, axis=1, keepdims=True)
        scores = (2.0 * dots - norms) / tau_ref[0]
        out = pl.ds(pl.multiple_of(block * half, half), half)
        for k, ref in enumerate((own_ref, near_ref, sparse_ref, dense_ref)):
            tile = scores[:, LANES * (k // 2):LANES * (k // 2) + LANES]
            top, bottom = tile[:half], tile[half:]
            if k % 2 == 0:
                ref[out, :] = jnp.where(low, top, pltpu.roll(bottom, 64, 1))
            else:
                ref[out, :] = jnp.where(low, pltpu.roll(top, 64, 1), bottom)


def score_call(me, tau, queries, keys, first, count):
    width = keys.shape[1]
    packed = jax.ShapeDtypeStruct((count * BLOCK // 2, LANES), jnp.float32)
    smem = pl.BlockSpec(memory_space=pltpu.SMEM)
    vmem = pl.BlockSpec(memory_space=pltpu.VMEM)
    return pl.pallas_call(
        functools.partial(scores_kernel, first, count),
        in_specs=[smem, smem, vmem, pl.BlockSpec(memory_space=pl.ANY)],
        out_specs=[vmem] * 4,
        out_shape=[packed] * 4,
        scratch_shapes=[pltpu.VMEM(queries.shape, queries.dtype), pltpu.VMEM((SLOTS, BLOCK, width), keys.dtype), pltpu.SemaphoreType.DMA((SLOTS,))],
        compiler_params=pltpu.CompilerParams(vmem_limit_bytes=30 * 1024 * 1024),
        cost_estimate=pl.CostEstimate(flops=2 * count * BLOCK * width * 256, bytes_accessed=count * BLOCK * width * 2, transcendentals=0),
        name="scores",
    )(me, tau, queries, keys)


def codes_kernel(m_ref, *refs):
    me = m_ref[0]
    for tok_ref, code_ref in zip(refs[:len(refs) // 2], refs[len(refs) // 2:]):
        tok = tok_ref[...]
        owner = sum((tok >= VOCAB_LOC * i).astype(jnp.int32) for i in (1, 2, 3))
        code = tok - owner * VOCAB_LOC + (owner ^ me) * VOCAB_LOC
        lane = lax.broadcasted_iota(jnp.int32, code.shape, 1)
        place = lane % BATCH
        clash = jnp.zeros_like(code)
        for d in range(1, BATCH):
            same = (code == pltpu.roll(code, LANES - d, 1)) & (place < BATCH - d)
            clash = clash | same.astype(jnp.int32)
        d = BATCH // 2
        while d:
            clash = clash | pltpu.roll(clash, LANES - d, 1)
            d //= 2
        any_clash = jnp.max(jnp.where(place == 0, clash, 0), axis=1, keepdims=True)
        code_ref[...] = code + jnp.where(place == 0, clash * CLASH, 0) * any_clash + jnp.where(place == 0, any_clash * FLAG, 0)


def codes_call(me, toks):
    shape = jax.ShapeDtypeStruct(toks[0].shape, jnp.int32)
    return pl.pallas_call(
        codes_kernel,
        in_specs=[pl.BlockSpec(memory_space=pltpu.SMEM)] + [pl.BlockSpec(memory_space=pltpu.VMEM)] * len(toks),
        out_specs=[pl.BlockSpec(memory_space=pltpu.VMEM)] * len(toks),
        out_shape=[shape] * len(toks),
        cost_estimate=pl.CostEstimate(flops=4_000_000, bytes_accessed=1 << 18, transcendentals=0),
        name="codes",
    )(me, *toks)


def fold(row, op):
    wide = jnp.broadcast_to(row, (8, LANES))
    return op(wide, pltpu.roll(wide, 64, 1))[:1]


def scatter_kernel(segments, n_codes, chunks, carried, s_ref, *refs):
    n_x = len(segments)
    code_refs, refs = refs[:n_codes], refs[n_codes:]
    x_refs, refs = refs[:n_x], refs[n_x:]
    if carried:
        prev_refs, refs = refs[:4], refs[4:]
    piece_refs = refs[:4]
    hist, e_ref, z_ref = refs[4:7]
    half = BLOCK // 2

    @pl.loop(0, hist.shape[0] // 320)
    def _(i):
        hist[pl.ds(pl.multiple_of(i * 320, 320), 320), :] = jnp.zeros((320, LANES), jnp.float32)

    z_ref[...] = jnp.zeros_like(z_ref)
    middle = (s_ref[0] == 1) | (s_ref[0] == 2)
    counts = [jnp.where(middle, x.shape[0] // half, 0) if seg[2] else x.shape[0] // half for x, seg in zip(x_refs, segments)]
    peak = jnp.full((8, LANES), -jnp.inf, jnp.float32)
    for x_ref, count in zip(x_refs, counts):
        def widen(block, peak):
            x = x_ref[pl.ds(pl.multiple_of(block * half, half), half), :]
            return jnp.maximum(peak, jnp.max(x.reshape(half // 8, 8, LANES), axis=0))

        peak = lax.fori_loop(0, count, widen, peak)
    top = fold(jnp.max(peak, axis=0, keepdims=True), jnp.maximum)

    for x_ref, (which, base, _), count in zip(x_refs, segments, counts):
        code_ref = code_refs[which]

        @pl.loop(0, count)
        def _(block):
            e = jnp.exp(x_ref[pl.ds(pl.multiple_of(block * half, half), half), :] - top)
            z_ref[...] += jnp.sum(e.reshape(half // 8, 8, LANES), axis=0)
            e_ref[:half] = e
            e_ref[half:] = pltpu.roll(e, 64, 1)

            @pl.loop(0, BLOCK // LANES)
            def _(group):
                row = pl.multiple_of(group * LANES, LANES)
                at = pl.multiple_of(base + block * BLOCK + group * LANES, LANES)
                ids_ref = code_ref.at[pl.ds(at, LANES)]
                rows_ref = e_ref.at[pl.ds(row, LANES)]
                head = ids_ref[0]

                @pl.when(head < FLAG)
                def _():
                    for b in range(0, LANES, BATCH):
                        ids = [ids_ref[b + i] for i in range(BATCH)]
                        new = [hist[pl.ds(ids[i], 1), :] + rows_ref[b + i:b + i + 1, :] for i in range(BATCH)]
                        for i in range(BATCH):
                            hist[pl.ds(ids[i], 1), :] = new[i]

                @pl.when(head >= FLAG)
                def _():
                    @pl.loop(0, LANES // BATCH)
                    def _(b):
                        mark = ids_ref[b * BATCH]
                        ids = [mark & (FLAG - 1)] + [ids_ref[b * BATCH + i] for i in range(1, BATCH)]
                        rows = rows_ref.at[pl.ds(pl.multiple_of(b * BATCH, BATCH), BATCH)]

                        @pl.when((mark & CLASH) == 0)
                        def _():
                            new = [hist[pl.ds(ids[i], 1), :] + rows[i:i + 1, :] for i in range(BATCH)]
                            for i in range(BATCH):
                                hist[pl.ds(ids[i], 1), :] = new[i]

                        @pl.when((mark & CLASH) != 0)
                        def _():
                            for i in range(BATCH):
                                hist[pl.ds(ids[i], 1), :] += rows[i:i + 1, :]

    z = fold(jnp.sum(z_ref[...], axis=0, keepdims=True), jnp.add)
    scale = held_scale = None
    if carried:
        held_top = prev_refs[0][PIECE + 1:PIECE + 2, :]
        both = jnp.maximum(top, held_top)
        scale, held_scale = jnp.exp(top - both), jnp.exp(held_top - both)
        z = z * scale + prev_refs[0][PIECE:PIECE + 1, :] * held_scale
        top = both
    meta = jnp.concatenate([z, top, jnp.zeros((META - 2, LANES), jnp.float32)], axis=0)
    size = PIECE // chunks

    def place(rel, c, at, rows, both):
        first = c * size + at
        lower = hist[pl.ds(pl.multiple_of(rel * VOCAB_LOC + first, 8), rows), :]
        low = lax.broadcasted_iota(jnp.int32, (rows, LANES), 1) < 64
        if both:
            value = jnp.where(low, lower, pltpu.roll(hist[pl.ds(pl.multiple_of(rel * VOCAB_LOC + PIECE + first, 8), rows), :], 64, 1))
        else:
            value = jnp.where(low, lower, 0.0)
        if carried:
            value = value * scale + prev_refs[rel][pl.ds(pl.multiple_of(first, 8), rows), :] * held_scale
        piece_refs[rel][pl.ds(pl.multiple_of(c * (size + META) + at, 8), rows), :] = value

    for rel in (3, 1, 2, 0):
        for c in range(chunks):
            full = min(size, UPPER - c * size)

            @pl.loop(0, full // STEP)
            def _(i):
                place(rel, c, i * STEP, STEP, True)

            rest = full % STEP
            if rest:
                place(rel, c, full - rest, rest, True)
            if full < size:
                place(rel, c, full, size - full, False)
            at = c * (size + META) + size
            piece_refs[rel][at:at + META, :] = meta


def scatter_call(s1, codes, xs, segments, prev, chunks):
    n_codes = len(codes)
    carried = prev is not None
    vmem = pl.BlockSpec(memory_space=pltpu.VMEM)
    smem = pl.BlockSpec(memory_space=pltpu.SMEM)
    piece = jax.ShapeDtypeStruct((PIECE + chunks * META, LANES), jnp.float32)
    n_keys = sum(2 * x.shape[0] for x in xs)
    return pl.pallas_call(
        functools.partial(scatter_kernel, segments, n_codes, chunks, carried),
        in_specs=[smem] + [smem] * n_codes + [vmem] * len(xs) + ([vmem] * 4 if carried else []),
        out_specs=[vmem] * 4,
        out_shape=[piece] * 4,
        scratch_shapes=[pltpu.VMEM((4 * VOCAB_LOC, LANES), jnp.float32), pltpu.VMEM((BLOCK, LANES), jnp.float32), pltpu.VMEM((8, LANES), jnp.float32)],
        compiler_params=pltpu.CompilerParams(vmem_limit_bytes=SCATTER_VMEM),
        cost_estimate=pl.CostEstimate(flops=n_keys * 1_000_000, bytes_accessed=n_keys * 512, transcendentals=n_keys * 64),
        name="scatter",
    )(s1, *codes, *xs, *(prev if carried else ()))


def merge_kernel(size, offsets, *refs):
    out_ref = refs[-1]
    tops = [r[o + size + 1:o + size + 2, :] for r, o in zip(refs, offsets)]
    top = functools.reduce(jnp.maximum, tops)
    scales = [jnp.exp(t - top) for t in tops]

    def total(at, count):
        parts = [r[pl.ds(pl.multiple_of(o + at, 8), count), :] * f for r, o, f in zip(refs, offsets, scales)]
        return functools.reduce(jnp.add, parts)

    @pl.loop(0, size // 256)
    def _(i):
        out_ref[pl.ds(pl.multiple_of(i * 256, 256), 256), :] = total(i * 256, 256)

    rest = total(size, META)
    out_ref[size:size + META, :] = jnp.where(lax.broadcasted_iota(jnp.int32, (META, LANES), 0) == 1, top, rest)


def merge_call(size, parts):
    vmem = pl.BlockSpec(memory_space=pltpu.VMEM)
    return pl.pallas_call(
        functools.partial(merge_kernel, size, tuple(c * (size + META) for _, c in parts)),
        in_specs=[vmem] * len(parts),
        out_specs=vmem,
        out_shape=jax.ShapeDtypeStruct((size + META, LANES), jnp.float32),
        compiler_params=pltpu.CompilerParams(vmem_limit_bytes=24 * 1024 * 1024),
        cost_estimate=pl.CostEstimate(flops=4_000_000_000, bytes_accessed=size * 2048, transcendentals=0),
        name="merge",
    )(*[a for a, _ in parts])


def final_kernel(chunks, s_ref, mix_ref, logits_ref, s0_ref, s1_ref, s2_ref, s3_ref, keep_ref, mate_ref, fromy_ref, *refs):
    far_refs, out_ref = refs[:chunks], refs[chunks]
    mix = mix_ref[0]
    end = (s_ref[0] == 0) | (s_ref[0] == 3)
    size = PIECE // chunks
    whole = (keep_ref, mate_ref, fromy_ref)
    metas = [r[PIECE:PIECE + META, :] for r in whole] + [far_refs[0][size:size + META, :]]
    tops = [t[1:2] for t in metas]
    tops[3] = jnp.where(end, tops[3], -jnp.inf)
    top = functools.reduce(jnp.maximum, tops)
    scales = [jnp.exp(t - top) for t in tops]
    z = sum(t[0:1] * f for t, f in zip(metas, scales))
    scales = [f * (mix / z) for f in scales]
    stats = [r[...] for r in (s0_ref, s1_ref, s2_ref, s3_ref)]
    lm_top = functools.reduce(jnp.maximum, [t[:, :1] for t in stats])
    total = sum(t[:, 64:65] * jnp.exp(t[:, :1] - lm_top) for t in stats)
    lm_scale = (1.0 - mix) / total

    def lm(at, count):
        return jnp.exp(logits_ref[:, at:at + count] - lm_top) * lm_scale

    for i in range(0, PIECE, LANES):
        far = far_refs[i // size][i % size:i % size + LANES, :]
        h = sum(r[i:i + LANES, :] * f for r, f in zip(whole, scales)) + far * scales[3]
        h = h.T
        out_ref[:, i:i + LANES] = jnp.log(h[:64] + lm(i, LANES))
        count = min(LANES, UPPER - i)
        if count > 0:
            out_ref[:, PIECE + i:PIECE + i + count] = jnp.log(h[64:, :count] + lm(PIECE + i, count))


def final_call(s1, mix, logits, stats, whole, far):
    vmem = pl.BlockSpec(memory_space=pltpu.VMEM)
    smem = pl.BlockSpec(memory_space=pltpu.SMEM)
    return pl.pallas_call(
        functools.partial(final_kernel, len(far)),
        in_specs=[smem, smem] + [vmem] * (8 + len(far)),
        out_specs=vmem,
        out_shape=jax.ShapeDtypeStruct(logits.shape, jnp.float32),
        compiler_params=pltpu.CompilerParams(vmem_limit_bytes=40 * 1024 * 1024),
        cost_estimate=pl.CostEstimate(flops=5_000_000_000, bytes_accessed=12 << 20, transcendentals=1 << 20),
        name="final",
    )(s1, mix, logits, *stats, *whole, *far)


NEAR = [(0, 1), (1, 0), (2, 3), (3, 2)]
FAR2 = [(0, 2), (3, 1)]
FAR1 = [(1, 2), (2, 1)]
INWARD = [(0, 1), (3, 2)]
ACROSS = [(1, 3), (2, 0)]
CHUNKS = 2


def solution(mesh):
    store_devs = mesh.shape["store"]

    def swap(x, axis, bit):
        return lax.ppermute(x, axis, [(i, i ^ bit) for i in range(4)])

    def local_step(queries, w_head, store_keys, store_tok, temperature, mix_weight):
        rows_loc = queries.shape[0] // store_devs
        s = lax.axis_index("store")
        m = lax.axis_index("model")
        s1, m1 = s.reshape(1), m.reshape(1)
        tau = temperature.reshape(1)
        blocks = store_keys.shape[0] // BLOCK
        n_a = FIRST * BLOCK
        size = PIECE // CHUNKS
        tok2 = store_tok.reshape(-1, LANES)

        toks = [lax.ppermute(tok2, "store", NEAR), lax.ppermute(tok2, "store", FAR2), lax.ppermute(tok2, "store", FAR1)]
        own_a, near_a, sparse_a, dense_a = score_call(s1, tau, queries, store_keys, 0, FIRST)
        far2_a = lax.ppermute(sparse_a, "store", FAR2)
        far1_a = lax.ppermute(sparse_a, "store", FAR1)
        got_a = lax.ppermute(near_a, "store", NEAR)
        own_b, near_b, sparse_b, dense_b = score_call(s1, tau, queries, store_keys, FIRST, blocks - FIRST)
        far2_b = lax.ppermute(sparse_b, "store", FAR2)
        far1_b = lax.ppermute(sparse_b, "store", FAR1)
        got_b = lax.ppermute(near_b, "store", NEAR)
        code_own, code_near, code_far2, code_far1 = [c.reshape(-1) for c in codes_call(m1, [tok2] + toks)]

        dense = scatter_call(s1, [code_own], [dense_a, dense_b], ((0, 0, False), (0, n_a, False)), None, CHUNKS)
        d_next = swap(dense[3], "model", 1)
        d_mate = swap(dense[1], "model", 1)
        d_y = []
        for c in range(CHUNKS):
            part = merge_call(size, [(dense[2], c), (d_next, c)])
            d_y.append(swap(part, "model", 2))

        xs = [own_a, own_b, got_a, far2_a, far1_a]
        segments = ((0, 0, False), (0, n_a, False), (1, 0, False), (2, 0, True), (3, 0, True))
        part = scatter_call(s1, [code_own, code_near, code_far2, code_far1], xs, segments, None, 1)
        xs = [got_b, far2_b, far1_b]
        segments = ((0, n_a, False), (1, n_a, True), (2, n_a, True))
        keep, mate, ynext, matey = scatter_call(s1, [code_near, code_far2, code_far1], xs, segments, part, 1)
        matey = swap(matey, "model", 1)
        mate = swap(mate, "model", 1)

        far = []
        for c in range(CHUNKS):
            plane = merge_call(size, [(dense[0], c), (d_mate, c), (d_y[c], 0)])
            inward = lax.ppermute(plane, "store", INWARD)
            pair = merge_call(size, [(plane, 0), (inward, 0)])
            far.append(lax.ppermute(pair, "store", ACROSS))

        ynext = merge_call(PIECE, [(ynext, 0), (matey, 0)])
        from_y = swap(ynext, "model", 2)

        my_rows = lax.dynamic_slice_in_dim(queries, s * rows_loc, rows_loc, axis=0)
        logits = lax.dot_general(my_rows, w_head, (((1,), (0,)), ((), ())), preferred_element_type=jnp.float32)
        lm_top = jnp.max(logits, axis=1, keepdims=True)
        lm_sum = jnp.sum(jnp.exp(logits - lm_top), axis=1, keepdims=True)
        stats = jnp.concatenate([jnp.broadcast_to(lm_top, (rows_loc, 64)), jnp.broadcast_to(lm_sum, (rows_loc, 64))], axis=1)
        stats = [stats] + [swap(stats, "model", k) for k in (1, 2, 3)]
        return final_call(s1, mix_weight.reshape(1), logits, stats, [keep, mate, from_y], far)

    return jax.shard_map(local_step, mesh=mesh, in_specs=(P("data", None), P(None, "model"), P(("store", "model"), None), P(("store", "model")), P(), P()), out_specs=P(("data", "store"), "model"), check_vma=False)
```

```python
import functools

import jax
import jax.numpy as jnp
from jax import lax
from jax.experimental import pallas as pl
from jax.experimental.pallas import tpu as pltpu
from jax.sharding import PartitionSpec as P


LANES = 128
BLOCK = 512
BATCH = 16
WIDE = 2
VOCAB_LOC = 8000
PIECE = 4096
FIRST = 6
META = 8
SLOTS = 4
OUT_GROUP = 2
TOK_ROWS = 64
MERGE_STEPS = 4
VMEM = 66_900_000
STEP = 976
UPPER = VOCAB_LOC - PIECE
FLAG = 1 << 16
CLASH = 1 << 17


def targets(me):
    left = me < 2
    return me, me ^ 1, jnp.where(left, 2, 1), jnp.where(left, 3, 0)


def codes_of(tok, me):
    owner = sum((tok >= VOCAB_LOC * i).astype(jnp.int32) for i in (1, 2, 3))
    code = tok - owner * VOCAB_LOC + (owner ^ me) * VOCAB_LOC
    lane = lax.broadcasted_iota(jnp.int32, code.shape, 1)
    place = lane % BATCH
    clash = jnp.zeros_like(code)
    for d in range(1, BATCH):
        same = (code == pltpu.roll(code, LANES - d, 1)) & (place < BATCH - d)
        clash = clash | same.astype(jnp.int32)
    d = BATCH // 2
    while d:
        clash = clash | pltpu.roll(clash, LANES - d, 1)
        d //= 2
    first = place == 0
    group = jnp.max(jnp.where(first, clash, 0), axis=1, keepdims=True)
    marks = FLAG + jnp.where(clash > 0, CLASH, 0)
    return code + jnp.where(first & (group > 0), marks, 0)


def scores_kernel(first, count, carried, s_ref, m_ref, tau_ref, q_hbm, k_hbm, tok_ref, *refs):
    refs = refs[2:] if carried else refs
    outs, refs = refs[:4], refs[4:]
    if not carried:
        code_hbm, refs = refs[0], refs[1:]
    q_ref, qs_ref, held, stage, code_i, code_f, sem, q_sem, out_sem, tok_sem = refs
    half = BLOCK // 2
    group = OUT_GROUP * half

    def fetch(block):
        slot = lax.rem(block, SLOTS)
        rows = pl.ds(pl.multiple_of((first + block) * BLOCK, BLOCK), BLOCK)
        return pltpu.make_async_copy(k_hbm.at[rows], held.at[slot], sem.at[slot])

    def save(g):
        copies = []
        for i, out in enumerate(outs):
            start = g * group + (0 if i in (1, 2) else first * half)
            rows = pl.ds(pl.multiple_of(start, half), group)
            copies.append(pltpu.make_async_copy(stage.at[i, pl.ds(pl.multiple_of(g * group, half), group)], out.at[rows], out_sem.at[i, g]))
        return copies

    load_q = pltpu.make_async_copy(q_hbm, q_ref, q_sem)
    load_q.start()
    fetch(0).start()
    tokens = []
    if not carried:
        code_i[...] = codes_of(tok_ref[...], m_ref[0])
        code_f[...] = code_i[...].astype(jnp.float32)
        at = {1: outs[1].shape[0] - TOK_ROWS, 2: outs[2].shape[0] - TOK_ROWS}
        tokens = [pltpu.make_async_copy(code_f, outs[i].at[pl.ds(at[i], TOK_ROWS)], tok_sem.at[i - 1]) for i in (1, 2)]
        tokens.append(pltpu.make_async_copy(code_i, code_hbm, tok_sem.at[2]))
        for copy in tokens:
            copy.start()
    load_q.wait()
    for block in range(1, SLOTS - 1):
        fetch(block).start()
    for k, z in enumerate(targets(s_ref[0])):
        qs_ref[64 * k:64 * k + 64, :] = q_ref[pl.ds(pl.multiple_of(z * 64, 64), 64), :]
    low = lax.broadcasted_iota(jnp.int32, (half, LANES), 1) < 64

    @pl.loop(0, count)
    def _(block):
        @pl.when(block + SLOTS - 1 < count)
        def _():
            fetch(block + SLOTS - 1).start()

        fetch(block).wait()
        keys = held[lax.rem(block, SLOTS)]
        dots = lax.dot_general(keys, qs_ref[...], (((1,), (1,)), ((), ())), preferred_element_type=jnp.float32)
        wide = keys.astype(jnp.float32)
        norms = jnp.sum(wide * wide, axis=1, keepdims=True)
        scores = (2.0 * dots - norms) / tau_ref[0]
        out = pl.ds(pl.multiple_of(block * half, half), half)
        for k in range(4):
            tile = scores[:, LANES * (k // 2):LANES * (k // 2) + LANES]
            top, bottom = tile[:half], tile[half:]
            if k % 2 == 0:
                stage[k, out, :] = jnp.where(low, top, pltpu.roll(bottom, 64, 1))
            else:
                stage[k, out, :] = jnp.where(low, pltpu.roll(top, 64, 1), bottom)

        @pl.when(lax.rem(block, OUT_GROUP) == OUT_GROUP - 1)
        def _():
            for copy in save(block // OUT_GROUP):
                copy.start()

    for g in range(count // OUT_GROUP):
        for copy in save(g):
            copy.wait()
    for copy in tokens:
        copy.wait()


def score_call(me, model, tau, queries, keys, tok2, first, count, prev):
    width = keys.shape[1]
    whole = keys.shape[0] // 2
    rows = count * BLOCK // 2
    smem = pl.BlockSpec(memory_space=pltpu.SMEM)
    hbm = pl.BlockSpec(memory_space=pltpu.HBM)
    sent = (rows + (0 if prev else TOK_ROWS), LANES)
    shapes = [(whole, LANES), sent, sent, (whole, LANES)]
    return pl.pallas_call(
        functools.partial(scores_kernel, first, count, bool(prev)),
        in_specs=[smem, smem, smem, hbm, hbm, pl.BlockSpec(memory_space=pltpu.VMEM)] + [hbm] * len(prev),
        out_specs=[hbm] * (4 if prev else 5),
        out_shape=[jax.ShapeDtypeStruct(shape, jnp.float32) for shape in shapes] + ([] if prev else [jax.ShapeDtypeStruct(tok2.shape, jnp.int32)]),
        scratch_shapes=[
            pltpu.VMEM(queries.shape, queries.dtype),
            pltpu.VMEM(queries.shape, queries.dtype),
            pltpu.VMEM((SLOTS, BLOCK, width), keys.dtype),
            pltpu.VMEM((4, rows, LANES), jnp.float32),
            pltpu.VMEM((TOK_ROWS, LANES), jnp.int32),
            pltpu.VMEM((TOK_ROWS, LANES), jnp.float32),
            pltpu.SemaphoreType.DMA((SLOTS,)),
            pltpu.SemaphoreType.DMA,
            pltpu.SemaphoreType.DMA((4, count // OUT_GROUP)),
            pltpu.SemaphoreType.DMA((3,)),
        ],
        input_output_aliases={6: 0, 7: 3} if prev else {},
        compiler_params=pltpu.CompilerParams(vmem_limit_bytes=VMEM),
        cost_estimate=pl.CostEstimate(flops=2 * count * BLOCK * width * 256, bytes_accessed=count * BLOCK * width * 2, transcendentals=0),
        name="scores",
    )(me, model, tau, queries, keys, tok2, *prev)


def fold(row, op):
    wide = jnp.broadcast_to(row, (8, LANES))
    return op(wide, pltpu.roll(wide, 64, 1))[:1]


def scatter_kernel(segments, n_codes, chunks, carried, s_ref, *refs):
    n_x = len(segments)
    code_hbms, refs = refs[:n_codes], refs[n_codes:]
    x_hbms, refs = refs[:n_x], refs[n_x:]
    if carried:
        prev_hbms, refs = refs[:4], refs[4:]
    piece_hbms, refs = refs[:4], refs[4:]
    hist, e_ref, z_ref, stage, sem, prev_sem, out_sem = refs[:7]
    x_refs, refs = refs[7:7 + n_x], refs[7 + n_x:]
    code_refs, refs = refs[:n_codes], refs[n_codes:]
    piece_refs = [stage.at[rel] for rel in range(4)]
    half = BLOCK // 2
    loads = [pltpu.make_async_copy(a.at[pl.ds(0, b.shape[0])], b, sem.at[i]) for i, (a, b) in enumerate(zip(x_hbms, x_refs))]
    loads += [pltpu.make_async_copy(a, b, sem.at[n_x + i]) for i, (a, b) in enumerate(zip(code_hbms, code_refs))]
    for load in loads:
        load.start()
    if carried:
        prev, = refs
        prev_refs = [prev.at[rel] for rel in range(4)]
        prev_loads = [pltpu.make_async_copy(a, prev.at[i], prev_sem.at[i]) for i, a in enumerate(prev_hbms)]
        for load in prev_loads:
            load.start()
    saves = [pltpu.make_async_copy(stage.at[rel], piece_hbms[rel], out_sem.at[rel]) for rel in range(4)]

    @pl.loop(0, hist.shape[0] // 320)
    def _(i):
        hist[pl.ds(pl.multiple_of(i * 320, 320), 320), :] = jnp.zeros((320, LANES), jnp.float32)

    z_ref[...] = jnp.zeros_like(z_ref)
    for load in loads:
        load.wait()
    middle = (s_ref[0] == 1) | (s_ref[0] == 2)
    counts = [jnp.where(middle, x.shape[0] // (WIDE * half), 0) if seg[2] else x.shape[0] // (WIDE * half) for x, seg in zip(x_refs, segments)]
    peak = jnp.full((8, LANES), -jnp.inf, jnp.float32)
    for x_ref, count in zip(x_refs, counts):
        def widen(block, peak):
            x = x_ref[pl.ds(pl.multiple_of(block * WIDE * half, WIDE * half), WIDE * half), :]
            return jnp.maximum(peak, jnp.max(x.reshape(WIDE * half // 8, 8, LANES), axis=0))

        peak = lax.fori_loop(0, count, widen, peak)
    top = fold(jnp.max(peak, axis=0, keepdims=True), jnp.maximum)

    for x_ref, (which, base, _), count in zip(x_refs, segments, counts):
        code_ref = code_refs[which]

        @pl.loop(0, count)
        def _(block):
            wide = pl.ds(pl.multiple_of(block * WIDE * half, WIDE * half), WIDE * half)
            e = jnp.exp(x_ref[wide, :] - top)
            z_ref[...] += jnp.sum(e.reshape(WIDE * half // 8, 8, LANES), axis=0)
            for i in range(WIDE):
                part = e[i * half:i * half + half]
                e_ref[i * BLOCK:i * BLOCK + half] = part
                e_ref[i * BLOCK + half:i * BLOCK + BLOCK] = pltpu.roll(part, 64, 1)

            @pl.loop(0, WIDE * BLOCK // LANES)
            def _(group):
                row = pl.multiple_of(group * LANES, LANES)
                at = pl.multiple_of(base + block * WIDE * BLOCK + group * LANES, LANES)
                rows_ref = e_ref.at[pl.ds(row, LANES)]
                head = code_ref[at]

                @pl.when(head < FLAG)
                def _():
                    for b in range(0, LANES, BATCH):
                        ids = [code_ref.at[pl.ds(b + i, code_ref.shape[0] - LANES + 1)][at] for i in range(BATCH)]
                        new = [hist[pl.ds(ids[i], 1), :] + rows_ref[b + i:b + i + 1, :] for i in range(BATCH)]
                        for i in range(BATCH):
                            hist[pl.ds(ids[i], 1), :] = new[i]

                @pl.when(head >= FLAG)
                def _():
                    @pl.loop(0, LANES // BATCH)
                    def _(b):
                        mark = code_ref[at + b * BATCH]
                        ids = [mark & (FLAG - 1)] + [code_ref[at + b * BATCH + i] for i in range(1, BATCH)]
                        rows = rows_ref.at[pl.ds(pl.multiple_of(b * BATCH, BATCH), BATCH)]

                        @pl.when((mark & CLASH) == 0)
                        def _():
                            new = [hist[pl.ds(ids[i], 1), :] + rows[i:i + 1, :] for i in range(BATCH)]
                            for i in range(BATCH):
                                hist[pl.ds(ids[i], 1), :] = new[i]

                        @pl.when((mark & CLASH) != 0)
                        def _():
                            for i in range(BATCH):
                                hist[pl.ds(ids[i], 1), :] += rows[i:i + 1, :]

    size = PIECE // chunks
    z = fold(jnp.sum(z_ref[...], axis=0, keepdims=True), jnp.add)
    scale = held_scale = None
    if carried:
        for load in prev_loads:
            load.wait()
        held_top = prev_refs[0][size + 1:size + 2, :]
        both = jnp.maximum(top, held_top)
        scale, held_scale = jnp.exp(top - both), jnp.exp(held_top - both)
        z = z * scale + prev_refs[0][size:size + 1, :] * held_scale
        top = both
    meta = jnp.concatenate([z, top, jnp.zeros((META - 2, LANES), jnp.float32)], axis=0)

    def place(rel, c, at, rows, both):
        first = c * size + at
        lower = hist[pl.ds(pl.multiple_of(rel * VOCAB_LOC + first, 8), rows), :]
        low = lax.broadcasted_iota(jnp.int32, (rows, LANES), 1) < 64
        if both:
            value = jnp.where(low, lower, pltpu.roll(hist[pl.ds(pl.multiple_of(rel * VOCAB_LOC + PIECE + first, 8), rows), :], 64, 1))
        else:
            value = jnp.where(low, lower, 0.0)
        if carried:
            value = value * scale + prev_refs[rel][pl.ds(pl.multiple_of(first + c * META, 8), rows), :] * held_scale
        piece_refs[rel][pl.ds(pl.multiple_of(c * (size + META) + at, 8), rows), :] = value

    for rel in (3, 1, 2, 0):
        for c in range(chunks):
            full = min(size, UPPER - c * size)

            @pl.loop(0, full // STEP)
            def _(i):
                place(rel, c, i * STEP, STEP, True)

            rest = full % STEP
            if rest:
                place(rel, c, full - rest, rest, True)
            if full < size:
                place(rel, c, full, size - full, False)
            at = c * (size + META) + size
            piece_refs[rel][at:at + META, :] = meta
        saves[rel].start()
    for save in saves:
        save.wait()


def scatter_call(s1, codes, xs, segments, prev):
    n_codes = len(codes)
    carried = prev is not None
    smem = pl.BlockSpec(memory_space=pltpu.SMEM)
    hbm = pl.BlockSpec(memory_space=pltpu.HBM)
    piece = jax.ShapeDtypeStruct((PIECE + CHUNKS * META, LANES), jnp.float32)
    n_keys = sum(2 * seg[0] for seg in segments)
    whole = pltpu.VMEM((4, *piece.shape), jnp.float32)
    return pl.pallas_call(
        functools.partial(scatter_kernel, tuple(seg[1:] for seg in segments), n_codes, CHUNKS, carried),
        in_specs=[smem] + [hbm] * (n_codes + len(xs) + (4 if carried else 0)),
        out_specs=[hbm] * 4,
        out_shape=[piece] * 4,
        scratch_shapes=[
            pltpu.VMEM((4 * VOCAB_LOC, LANES), jnp.float32),
            pltpu.VMEM((WIDE * BLOCK, LANES), jnp.float32),
            pltpu.VMEM((8, LANES), jnp.float32),
            whole,
            pltpu.SemaphoreType.DMA((len(xs) + n_codes,)),
            pltpu.SemaphoreType.DMA((4,)),
            pltpu.SemaphoreType.DMA((4,)),
        ]
        + [pltpu.VMEM((seg[0], LANES), jnp.float32) for seg in segments]
        + [pltpu.SMEM(c.shape, jnp.int32) for c in codes]
        + ([whole] if carried else []),
        compiler_params=pltpu.CompilerParams(vmem_limit_bytes=VMEM),
        cost_estimate=pl.CostEstimate(flops=n_keys * 1_000_000, bytes_accessed=n_keys * 512, transcendentals=n_keys * 64),
        name="scatter",
    )(s1, *codes, *xs, *(prev if carried else ()))


def merge_kernel(size, offsets, *refs):
    n = len(offsets)
    srcs, out_hbm, (stage, sem, out_sem, *bufs) = refs[:n], refs[n], refs[n + 1:]
    step = size // MERGE_STEPS
    parts = [(size, META)] + [(i * step, step) for i in range(MERGE_STEPS)]
    loads = [[pltpu.make_async_copy(r.at[pl.ds(o + at, rows)], b.at[pl.ds(at, rows)], sem.at[i, j]) for i, (r, o, b) in enumerate(zip(srcs, offsets, bufs))] for j, (at, rows) in enumerate(parts)]
    saves = [pltpu.make_async_copy(stage.at[pl.ds(at, rows)], out_hbm.at[pl.ds(at, rows)], out_sem.at[j]) for j, (at, rows) in enumerate(parts)]
    for group in loads:
        for load in group:
            load.start()
    for j, (at, rows) in enumerate(parts):
        for load in loads[j]:
            load.wait()
        if j == 0:
            tops = [b[size + 1:size + 2, :] for b in bufs]
            top = functools.reduce(jnp.maximum, tops)
            scales = [jnp.exp(t - top) for t in tops]
        total = functools.reduce(jnp.add, [b[at:at + rows, :] * f for b, f in zip(bufs, scales)])
        if j == 0:
            total = jnp.where(lax.broadcasted_iota(jnp.int32, (META, LANES), 0) == 1, top, total)
        stage[at:at + rows, :] = total
        saves[j].start()
    for save in saves:
        save.wait()


def merge_call(size, parts):
    hbm = pl.BlockSpec(memory_space=pltpu.HBM)
    shape = (size + META, LANES)
    return pl.pallas_call(
        functools.partial(merge_kernel, size, tuple(c * (size + META) for _, c in parts)),
        in_specs=[hbm] * len(parts),
        out_specs=hbm,
        out_shape=jax.ShapeDtypeStruct(shape, jnp.float32),
        scratch_shapes=[pltpu.VMEM(shape, jnp.float32), pltpu.SemaphoreType.DMA((len(parts), MERGE_STEPS + 1)), pltpu.SemaphoreType.DMA((MERGE_STEPS + 1,))] + [pltpu.VMEM(shape, jnp.float32)] * len(parts),
        compiler_params=pltpu.CompilerParams(vmem_limit_bytes=VMEM),
        cost_estimate=pl.CostEstimate(flops=4_000_000_000, bytes_accessed=size * 2048, transcendentals=0),
        name="merge",
    )(*[a for a, _ in parts])


def final_kernel(chunks, s_ref, mix_ref, logits_ref, s0_ref, s1_ref, s2_ref, s3_ref, keep_ref, mate_ref, *refs):
    y_refs, far_refs, out_ref = refs[:chunks], refs[chunks:2 * chunks], refs[2 * chunks]
    mix = mix_ref[0]
    end = (s_ref[0] == 0) | (s_ref[0] == 3)
    size = PIECE // chunks
    metas = [r[size:size + META, :] for r in (keep_ref, mate_ref, y_refs[0], far_refs[0])]
    tops = [t[1:2] for t in metas]
    tops[3] = jnp.where(end, tops[3], -jnp.inf)
    top = functools.reduce(jnp.maximum, tops)
    scales = [jnp.exp(t - top) for t in tops]
    z = sum(t[0:1] * f for t, f in zip(metas, scales))
    scales = [f * (mix / z) for f in scales]
    stats = [r[...] for r in (s0_ref, s1_ref, s2_ref, s3_ref)]
    lm_top = functools.reduce(jnp.maximum, [t[:, :1] for t in stats])
    total = sum(t[:, 64:65] * jnp.exp(t[:, :1] - lm_top) for t in stats)
    lm_scale = (1.0 - mix) / total

    def lm(at, count):
        return jnp.exp(logits_ref[:, at:at + count] - lm_top) * lm_scale

    for i in range(0, PIECE, LANES):
        c, at = i // size, i % size
        base = c * (size + META) + at
        parts = [keep_ref[base:base + LANES, :], mate_ref[base:base + LANES, :], y_refs[c][at:at + LANES, :], far_refs[c][at:at + LANES, :]]
        h = sum(p * f for p, f in zip(parts, scales))
        h = h.T
        out_ref[:, i:i + LANES] = jnp.log(h[:64] + lm(i, LANES))
        count = min(LANES, UPPER - i)
        if count > 0:
            out_ref[:, PIECE + i:PIECE + i + count] = jnp.log(h[64:, :count] + lm(PIECE + i, count))


def final_call(s1, mix, logits, stats, keep, mate, from_y, far):
    vmem = pl.BlockSpec(memory_space=pltpu.VMEM)
    smem = pl.BlockSpec(memory_space=pltpu.SMEM)
    return pl.pallas_call(
        functools.partial(final_kernel, len(far)),
        in_specs=[smem, smem] + [vmem] * (7 + 2 * len(far)),
        out_specs=vmem,
        out_shape=jax.ShapeDtypeStruct(logits.shape, jnp.float32),
        compiler_params=pltpu.CompilerParams(vmem_limit_bytes=40 * 1024 * 1024),
        cost_estimate=pl.CostEstimate(flops=5_000_000_000, bytes_accessed=12 << 20, transcendentals=1 << 20),
        name="final",
    )(s1, mix, logits, *stats, keep, mate, *from_y, *far)


NEAR = [(0, 1), (1, 0), (2, 3), (3, 2)]
FAR2 = [(0, 2), (3, 1)]
FAR1 = [(1, 2), (2, 1)]
INWARD = [(0, 1), (3, 2)]
ACROSS = [(1, 3), (2, 0)]
CHUNKS = 2


def solution(mesh):
    store_devs = mesh.shape["store"]

    def swap(x, axis, bit):
        return lax.ppermute(x, axis, [(i, i ^ bit) for i in range(4)])

    def local_step(queries, w_head, store_keys, store_tok, temperature, mix_weight):
        rows_loc = queries.shape[0] // store_devs
        s = lax.axis_index("store")
        m = lax.axis_index("model")
        s1, m1 = s.reshape(1), m.reshape(1)
        tau = temperature.reshape(1)
        blocks = store_keys.shape[0] // BLOCK
        n_a = FIRST * BLOCK
        size = PIECE // CHUNKS
        tok2 = store_tok.reshape(-1, LANES)

        toks = [lax.ppermute(tok2, "store", NEAR), lax.ppermute(tok2, "store", FAR2), lax.ppermute(tok2, "store", FAR1)]
        rows_a = n_a // 2
        rows_b = store_keys.shape[0] // 2 - rows_a
        own, near_a, sparse_a, dense, code_own = score_call(s1, m1, tau, queries, store_keys, tok2, 0, FIRST, [])
        far2_a = lax.ppermute(sparse_a, "store", FAR2)
        far1_a = lax.ppermute(sparse_a, "store", FAR1)
        near_a = lax.ppermute(near_a, "store", NEAR)
        own, near_b, sparse_b, dense = score_call(s1, m1, tau, queries, store_keys, tok2, FIRST, blocks - FIRST, [own, dense])
        far2_b = lax.ppermute(sparse_b, "store", FAR2)
        far1_b = lax.ppermute(sparse_b, "store", FAR1)
        near_b = lax.ppermute(near_b, "store", NEAR)
        code_own = code_own.reshape(-1)
        code_far2, code_far1, code_near = [x[-TOK_ROWS:].astype(jnp.int32).reshape(-1) for x in (far2_a, far1_a, near_a)]

        dense = scatter_call(s1, [code_own], [dense], ((rows_a + rows_b, 0, 0, False),), None)
        d_next = swap(dense[3], "model", 1)
        d_mate = swap(dense[1], "model", 1)
        d_y = []
        for c in range(CHUNKS):
            part = merge_call(size, [(dense[2], c), (d_next, c)])
            d_y.append(swap(part, "model", 2))

        segments = ((rows_a + rows_b, 0, 0, False), (rows_a, 1, 0, False), (rows_a, 2, 0, True), (rows_a, 3, 0, True))
        part = scatter_call(s1, [code_own, code_near, code_far2, code_far1], [own, near_a, far2_a, far1_a], segments, None)
        segments = ((rows_b, 0, n_a, False), (rows_b, 1, n_a, True), (rows_b, 2, n_a, True))
        keep, mate, ynext, matey = scatter_call(s1, [code_near, code_far2, code_far1], [near_b, far2_b, far1_b], segments, part)
        matey = swap(matey, "model", 1)
        mate = swap(mate, "model", 1)

        far = []
        for c in range(CHUNKS):
            plane = merge_call(size, [(dense[0], c), (d_mate, c), (d_y[c], 0)])
            inward = lax.ppermute(plane, "store", INWARD)
            pair = merge_call(size, [(plane, 0), (inward, 0)])
            far.append(lax.ppermute(pair, "store", ACROSS))

        from_y = []
        for c in range(CHUNKS):
            part = merge_call(size, [(ynext, c), (matey, c)])
            from_y.append(swap(part, "model", 2))

        my_rows = lax.dynamic_slice_in_dim(queries, s * rows_loc, rows_loc, axis=0)
        logits = lax.dot_general(my_rows, w_head, (((1,), (0,)), ((), ())), preferred_element_type=jnp.float32)
        lm_top = jnp.max(logits, axis=1, keepdims=True)
        lm_sum = jnp.sum(jnp.exp(logits - lm_top), axis=1, keepdims=True)
        stats = jnp.concatenate([jnp.broadcast_to(lm_top, (rows_loc, 64)), jnp.broadcast_to(lm_sum, (rows_loc, 64))], axis=1)
        stats = [stats] + [swap(stats, "model", k) for k in (1, 2, 3)]
        return final_call(s1, mix_weight.reshape(1), logits, stats, keep, mate, from_y, far)

    return jax.shard_map(local_step, mesh=mesh, in_specs=(P("data", None), P(None, "model"), P(("store", "model"), None), P(("store", "model")), P(), P()), out_specs=P(("data", "store"), "model"), check_vma=False)
```

```python
import functools

import jax
import jax.numpy as jnp
from jax import lax
from jax.experimental import pallas as pl
from jax.experimental.pallas import tpu as pltpu
from jax.sharding import PartitionSpec as P


LANES = 128
BLOCK = 512
BATCH = 16
WIDE = 2
VOCAB_LOC = 8000
PIECE = 4096
FIRST = 8
META = 8
SLOTS = 4
OUT_GROUP = 2
TOK_ROWS = 64
MERGE_STEPS = 4
VMEM = 66_900_000
STEP = 976
UPPER = VOCAB_LOC - PIECE
FLAG = 1 << 16
CLASH = 1 << 17


def targets(me):
    left = me < 2
    return me, me ^ 1, jnp.where(left, 2, 1), jnp.where(left, 3, 0)


def codes_of(tok, me):
    owner = sum((tok >= VOCAB_LOC * i).astype(jnp.int32) for i in (1, 2, 3))
    code = tok - owner * VOCAB_LOC + (owner ^ me) * VOCAB_LOC
    lane = lax.broadcasted_iota(jnp.int32, code.shape, 1)
    place = lane % BATCH
    clash = jnp.zeros_like(code)
    for d in range(1, BATCH):
        same = (code == pltpu.roll(code, LANES - d, 1)) & (place < BATCH - d)
        clash = clash | same.astype(jnp.int32)
    d = BATCH // 2
    while d:
        clash = clash | pltpu.roll(clash, LANES - d, 1)
        d //= 2
    first = place == 0
    group = jnp.max(jnp.where(first, clash, 0), axis=1, keepdims=True)
    marks = FLAG + jnp.where(clash > 0, CLASH, 0)
    return code + jnp.where(first & (group > 0), marks, 0)


def scores_kernel(first, count, carried, s_ref, m_ref, tau_ref, q_hbm, k_hbm, tok_ref, *refs):
    refs = refs[2:] if carried else refs
    outs, refs = refs[:4], refs[4:]
    if not carried:
        code_hbm, refs = refs[0], refs[1:]
    q_ref, qs_ref, held, stage, code_i, code_f, sem, q_sem, out_sem, tok_sem = refs
    half = BLOCK // 2
    group = OUT_GROUP * half

    def fetch(block):
        slot = lax.rem(block, SLOTS)
        rows = pl.ds(pl.multiple_of((first + block) * BLOCK, BLOCK), BLOCK)
        return pltpu.make_async_copy(k_hbm.at[rows], held.at[slot], sem.at[slot])

    def save(g):
        copies = []
        for i, out in enumerate(outs):
            start = g * group + (0 if i in (1, 2) else first * half)
            rows = pl.ds(pl.multiple_of(start, half), group)
            copies.append(pltpu.make_async_copy(stage.at[i, pl.ds(pl.multiple_of(g * group, half), group)], out.at[rows], out_sem.at[i, g]))
        return copies

    load_q = pltpu.make_async_copy(q_hbm, q_ref, q_sem)
    load_q.start()
    fetch(0).start()
    tokens = []
    if not carried:
        code_i[...] = codes_of(tok_ref[...], m_ref[0])
        code_f[...] = code_i[...].astype(jnp.float32)
        at = {1: outs[1].shape[0] - TOK_ROWS, 2: outs[2].shape[0] - TOK_ROWS}
        tokens = [pltpu.make_async_copy(code_f, outs[i].at[pl.ds(at[i], TOK_ROWS)], tok_sem.at[i - 1]) for i in (1, 2)]
        tokens.append(pltpu.make_async_copy(code_i, code_hbm, tok_sem.at[2]))
        for copy in tokens:
            copy.start()
    load_q.wait()
    for block in range(1, SLOTS - 1):
        fetch(block).start()
    for k, z in enumerate(targets(s_ref[0])):
        qs_ref[64 * k:64 * k + 64, :] = q_ref[pl.ds(pl.multiple_of(z * 64, 64), 64), :]
    low = lax.broadcasted_iota(jnp.int32, (half, LANES), 1) < 64

    @pl.loop(0, count)
    def _(block):
        @pl.when(block + SLOTS - 1 < count)
        def _():
            fetch(block + SLOTS - 1).start()

        fetch(block).wait()
        keys = held[lax.rem(block, SLOTS)]
        dots = lax.dot_general(keys, qs_ref[...], (((1,), (1,)), ((), ())), preferred_element_type=jnp.float32)
        wide = keys.astype(jnp.float32)
        norms = jnp.sum(wide * wide, axis=1, keepdims=True)
        scores = (2.0 * dots - norms) / tau_ref[0]
        out = pl.ds(pl.multiple_of(block * half, half), half)
        for k in range(4):
            tile = scores[:, LANES * (k // 2):LANES * (k // 2) + LANES]
            top, bottom = tile[:half], tile[half:]
            if k % 2 == 0:
                stage[k, out, :] = jnp.where(low, top, pltpu.roll(bottom, 64, 1))
            else:
                stage[k, out, :] = jnp.where(low, pltpu.roll(top, 64, 1), bottom)

        @pl.when(lax.rem(block, OUT_GROUP) == OUT_GROUP - 1)
        def _():
            for copy in save(block // OUT_GROUP):
                copy.start()

    for g in range(count // OUT_GROUP):
        for copy in save(g):
            copy.wait()
    for copy in tokens:
        copy.wait()


def score_call(me, model, tau, queries, keys, tok2, first, count, prev):
    width = keys.shape[1]
    whole = keys.shape[0] // 2
    rows = count * BLOCK // 2
    smem = pl.BlockSpec(memory_space=pltpu.SMEM)
    hbm = pl.BlockSpec(memory_space=pltpu.HBM)
    sent = (rows + (0 if prev else TOK_ROWS), LANES)
    shapes = [(whole, LANES), sent, sent, (whole, LANES)]
    return pl.pallas_call(
        functools.partial(scores_kernel, first, count, bool(prev)),
        in_specs=[smem, smem, smem, hbm, hbm, pl.BlockSpec(memory_space=pltpu.VMEM)] + [hbm] * len(prev),
        out_specs=[hbm] * (4 if prev else 5),
        out_shape=[jax.ShapeDtypeStruct(shape, jnp.float32) for shape in shapes] + ([] if prev else [jax.ShapeDtypeStruct(tok2.shape, jnp.int32)]),
        scratch_shapes=[
            pltpu.VMEM(queries.shape, queries.dtype),
            pltpu.VMEM(queries.shape, queries.dtype),
            pltpu.VMEM((SLOTS, BLOCK, width), keys.dtype),
            pltpu.VMEM((4, rows, LANES), jnp.float32),
            pltpu.VMEM((TOK_ROWS, LANES), jnp.int32),
            pltpu.VMEM((TOK_ROWS, LANES), jnp.float32),
            pltpu.SemaphoreType.DMA((SLOTS,)),
            pltpu.SemaphoreType.DMA,
            pltpu.SemaphoreType.DMA((4, count // OUT_GROUP)),
            pltpu.SemaphoreType.DMA((3,)),
        ],
        input_output_aliases={6: 0, 7: 3} if prev else {},
        compiler_params=pltpu.CompilerParams(vmem_limit_bytes=VMEM),
        cost_estimate=pl.CostEstimate(flops=2 * count * BLOCK * width * 256, bytes_accessed=count * BLOCK * width * 2, transcendentals=0),
        name="scores",
    )(me, model, tau, queries, keys, tok2, *prev)


def ids_kernel(*refs):
    n = len(refs) - 5
    srcs, (out_hbm, raw, ids, sem, out_sem) = refs[:n], refs[n:]
    loads = [pltpu.make_async_copy(r.at[pl.ds(r.shape[0] - TOK_ROWS, TOK_ROWS)], raw.at[i], sem.at[i]) for i, r in enumerate(srcs)]
    saves = [pltpu.make_async_copy(ids.at[i], out_hbm.at[pl.ds(i * TOK_ROWS, TOK_ROWS)], out_sem.at[i]) for i in range(n)]
    for load in loads:
        load.start()
    for i in range(n):
        loads[i].wait()
        ids[i] = raw[i].astype(jnp.int32)
        saves[i].start()
    for save in saves:
        save.wait()


def ids_call(arrays):
    n = len(arrays)
    hbm = pl.BlockSpec(memory_space=pltpu.HBM)
    shape = (n, TOK_ROWS, LANES)
    return pl.pallas_call(
        ids_kernel,
        in_specs=[hbm] * n,
        out_specs=hbm,
        out_shape=jax.ShapeDtypeStruct((n * TOK_ROWS, LANES), jnp.int32),
        scratch_shapes=[pltpu.VMEM(shape, jnp.float32), pltpu.VMEM(shape, jnp.int32), pltpu.SemaphoreType.DMA((n,)), pltpu.SemaphoreType.DMA((n,))],
        compiler_params=pltpu.CompilerParams(vmem_limit_bytes=VMEM),
        cost_estimate=pl.CostEstimate(flops=1_000_000, bytes_accessed=1 << 18, transcendentals=0),
        name="ids",
    )(*arrays)


def fold(row, op):
    wide = jnp.broadcast_to(row, (8, LANES))
    return op(wide, pltpu.roll(wide, 64, 1))[:1]


def scatter_kernel(segments, n_codes, chunks, carried, s_ref, *refs):
    n_x = len(segments)
    code_hbms, refs = refs[:n_codes], refs[n_codes:]
    x_hbms, refs = refs[:n_x], refs[n_x:]
    if carried:
        prev_hbms, refs = refs[:4], refs[4:]
    piece_hbms, refs = refs[:4], refs[4:]
    hist, e_ref, z_ref, stage, sem, prev_sem, out_sem = refs[:7]
    x_refs, refs = refs[7:7 + n_x], refs[7 + n_x:]
    code_refs, refs = refs[:n_codes], refs[n_codes:]
    piece_refs = [stage.at[rel] for rel in range(4)]
    half = BLOCK // 2
    loads = [pltpu.make_async_copy(a.at[pl.ds(0, b.shape[0])], b, sem.at[i]) for i, (a, b) in enumerate(zip(x_hbms, x_refs))]
    loads += [pltpu.make_async_copy(a, b, sem.at[n_x + i]) for i, (a, b) in enumerate(zip(code_hbms, code_refs))]
    for load in loads:
        load.start()
    if carried:
        prev, = refs
        prev_refs = [prev.at[rel] for rel in range(4)]
        prev_loads = [pltpu.make_async_copy(a, prev.at[i], prev_sem.at[i]) for i, a in enumerate(prev_hbms)]
        for load in prev_loads:
            load.start()
    saves = [pltpu.make_async_copy(stage.at[rel], piece_hbms[rel], out_sem.at[rel]) for rel in range(4)]

    @pl.loop(0, hist.shape[0] // 320)
    def _(i):
        hist[pl.ds(pl.multiple_of(i * 320, 320), 320), :] = jnp.zeros((320, LANES), jnp.float32)

    z_ref[...] = jnp.zeros_like(z_ref)
    for load in loads:
        load.wait()
    middle = (s_ref[0] == 1) | (s_ref[0] == 2)
    counts = [jnp.where(middle, x.shape[0] // (WIDE * half), 0) if seg[2] else x.shape[0] // (WIDE * half) for x, seg in zip(x_refs, segments)]
    peak = jnp.full((8, LANES), -jnp.inf, jnp.float32)
    for x_ref, count in zip(x_refs, counts):
        def widen(block, peak):
            x = x_ref[pl.ds(pl.multiple_of(block * WIDE * half, WIDE * half), WIDE * half), :]
            return jnp.maximum(peak, jnp.max(x.reshape(WIDE * half // 8, 8, LANES), axis=0))

        peak = lax.fori_loop(0, count, widen, peak)
    top = fold(jnp.max(peak, axis=0, keepdims=True), jnp.maximum)

    for x_ref, (which, base, _), count in zip(x_refs, segments, counts):
        code_ref = code_refs[which]

        @pl.loop(0, count)
        def _(block):
            wide = pl.ds(pl.multiple_of(block * WIDE * half, WIDE * half), WIDE * half)
            e = jnp.exp(x_ref[wide, :] - top)
            z_ref[...] += jnp.sum(e.reshape(WIDE * half // 8, 8, LANES), axis=0)
            for i in range(WIDE):
                part = e[i * half:i * half + half]
                e_ref[i * BLOCK:i * BLOCK + half] = part
                e_ref[i * BLOCK + half:i * BLOCK + BLOCK] = pltpu.roll(part, 64, 1)

            @pl.loop(0, WIDE * BLOCK // LANES)
            def _(group):
                row = pl.multiple_of(group * LANES, LANES)
                at = pl.multiple_of(base + block * WIDE * BLOCK + group * LANES, LANES)
                rows_ref = e_ref.at[pl.ds(row, LANES)]
                head = code_ref[at]

                @pl.when(head < FLAG)
                def _():
                    for b in range(0, LANES, BATCH):
                        ids = [code_ref.at[pl.ds(b + i, code_ref.shape[0] - LANES + 1)][at] for i in range(BATCH)]
                        new = [hist[pl.ds(ids[i], 1), :] + rows_ref[b + i:b + i + 1, :] for i in range(BATCH)]
                        for i in range(BATCH):
                            hist[pl.ds(ids[i], 1), :] = new[i]

                @pl.when(head >= FLAG)
                def _():
                    @pl.loop(0, LANES // BATCH)
                    def _(b):
                        mark = code_ref[at + b * BATCH]
                        ids = [mark & (FLAG - 1)] + [code_ref[at + b * BATCH + i] for i in range(1, BATCH)]
                        rows = rows_ref.at[pl.ds(pl.multiple_of(b * BATCH, BATCH), BATCH)]

                        @pl.when((mark & CLASH) == 0)
                        def _():
                            new = [hist[pl.ds(ids[i], 1), :] + rows[i:i + 1, :] for i in range(BATCH)]
                            for i in range(BATCH):
                                hist[pl.ds(ids[i], 1), :] = new[i]

                        @pl.when((mark & CLASH) != 0)
                        def _():
                            for i in range(BATCH):
                                hist[pl.ds(ids[i], 1), :] += rows[i:i + 1, :]

    size = PIECE // chunks
    z = fold(jnp.sum(z_ref[...], axis=0, keepdims=True), jnp.add)
    scale = held_scale = None
    if carried:
        for load in prev_loads:
            load.wait()
        held_top = prev_refs[0][size + 1:size + 2, :]
        both = jnp.maximum(top, held_top)
        scale, held_scale = jnp.exp(top - both), jnp.exp(held_top - both)
        z = z * scale + prev_refs[0][size:size + 1, :] * held_scale
        top = both
    meta = jnp.concatenate([z, top, jnp.zeros((META - 2, LANES), jnp.float32)], axis=0)

    def place(rel, c, at, rows, both):
        first = c * size + at
        lower = hist[pl.ds(pl.multiple_of(rel * VOCAB_LOC + first, 8), rows), :]
        low = lax.broadcasted_iota(jnp.int32, (rows, LANES), 1) < 64
        if both:
            value = jnp.where(low, lower, pltpu.roll(hist[pl.ds(pl.multiple_of(rel * VOCAB_LOC + PIECE + first, 8), rows), :], 64, 1))
        else:
            value = jnp.where(low, lower, 0.0)
        if carried:
            value = value * scale + prev_refs[rel][pl.ds(pl.multiple_of(first + c * META, 8), rows), :] * held_scale
        piece_refs[rel][pl.ds(pl.multiple_of(c * (size + META) + at, 8), rows), :] = value

    for rel in (3, 1, 2, 0):
        for c in range(chunks):
            full = min(size, UPPER - c * size)

            @pl.loop(0, full // STEP)
            def _(i):
                place(rel, c, i * STEP, STEP, True)

            rest = full % STEP
            if rest:
                place(rel, c, full - rest, rest, True)
            if full < size:
                place(rel, c, full, size - full, False)
            at = c * (size + META) + size
            piece_refs[rel][at:at + META, :] = meta
        saves[rel].start()
    for save in saves:
        save.wait()


def scatter_call(s1, codes, xs, segments, prev):
    n_codes = len(codes)
    carried = prev is not None
    smem = pl.BlockSpec(memory_space=pltpu.SMEM)
    hbm = pl.BlockSpec(memory_space=pltpu.HBM)
    piece = jax.ShapeDtypeStruct((PIECE + CHUNKS * META, LANES), jnp.float32)
    n_keys = sum(2 * seg[0] for seg in segments)
    whole = pltpu.VMEM((4, *piece.shape), jnp.float32)
    return pl.pallas_call(
        functools.partial(scatter_kernel, tuple(seg[1:] for seg in segments), n_codes, CHUNKS, carried),
        in_specs=[smem] + [hbm] * (n_codes + len(xs) + (4 if carried else 0)),
        out_specs=[hbm] * 4,
        out_shape=[piece] * 4,
        scratch_shapes=[
            pltpu.VMEM((4 * VOCAB_LOC, LANES), jnp.float32),
            pltpu.VMEM((WIDE * BLOCK, LANES), jnp.float32),
            pltpu.VMEM((8, LANES), jnp.float32),
            whole,
            pltpu.SemaphoreType.DMA((len(xs) + n_codes,)),
            pltpu.SemaphoreType.DMA((4,)),
            pltpu.SemaphoreType.DMA((4,)),
        ]
        + [pltpu.VMEM((seg[0], LANES), jnp.float32) for seg in segments]
        + [pltpu.SMEM(c.shape, jnp.int32) for c in codes]
        + ([whole] if carried else []),
        compiler_params=pltpu.CompilerParams(vmem_limit_bytes=VMEM),
        cost_estimate=pl.CostEstimate(flops=n_keys * 1_000_000, bytes_accessed=n_keys * 512, transcendentals=n_keys * 64),
        name="scatter",
    )(s1, *codes, *xs, *(prev if carried else ()))


def merge_kernel(size, groups, *refs):
    n, n_out = len(groups[0]), len(groups)
    srcs, outs, refs = refs[:n], refs[n:n + n_out], refs[n + n_out:]
    stages, sem, out_sem, bufs = refs[:n_out], refs[n_out], refs[n_out + 1], refs[n_out + 2:]
    step = size // MERGE_STEPS
    parts = [(size, META)] + [(i * step, step) for i in range(MERGE_STEPS)]
    work = []
    for g, offsets in enumerate(groups):
        mine = bufs[g * n:g * n + n]
        loads = [[pltpu.make_async_copy(r.at[pl.ds(o + at, rows)], b.at[pl.ds(at, rows)], sem.at[g, i, j]) for i, (r, o, b) in enumerate(zip(srcs, offsets, mine))] for j, (at, rows) in enumerate(parts)]
        saves = [pltpu.make_async_copy(stages[g].at[pl.ds(at, rows)], outs[g].at[pl.ds(at, rows)], out_sem.at[g, j]) for j, (at, rows) in enumerate(parts)]
        work.append((mine, loads, saves, stages[g]))
    for _, loads, _, _ in work:
        for group in loads:
            for load in group:
                load.start()
    for mine, loads, saves, stage in work:
        for j, (at, rows) in enumerate(parts):
            for load in loads[j]:
                load.wait()
            if j == 0:
                tops = [b[size + 1:size + 2, :] for b in mine]
                top = functools.reduce(jnp.maximum, tops)
                scales = [jnp.exp(t - top) for t in tops]
            total = functools.reduce(jnp.add, [b[at:at + rows, :] * f for b, f in zip(mine, scales)])
            if j == 0:
                total = jnp.where(lax.broadcasted_iota(jnp.int32, (META, LANES), 0) == 1, top, total)
            stage[at:at + rows, :] = total
            saves[j].start()
    for _, _, saves, _ in work:
        for save in saves:
            save.wait()


def merge_call(size, arrays, groups):
    hbm = pl.BlockSpec(memory_space=pltpu.HBM)
    shape = (size + META, LANES)
    n, n_out = len(arrays), len(groups)
    return pl.pallas_call(
        functools.partial(merge_kernel, size, tuple(tuple(c * (size + META) for c in group) for group in groups)),
        in_specs=[hbm] * n,
        out_specs=[hbm] * n_out,
        out_shape=[jax.ShapeDtypeStruct(shape, jnp.float32)] * n_out,
        scratch_shapes=[pltpu.VMEM(shape, jnp.float32)] * n_out
        + [pltpu.SemaphoreType.DMA((n_out, n, MERGE_STEPS + 1)), pltpu.SemaphoreType.DMA((n_out, MERGE_STEPS + 1))]
        + [pltpu.VMEM(shape, jnp.float32)] * (n * n_out),
        compiler_params=pltpu.CompilerParams(vmem_limit_bytes=VMEM),
        cost_estimate=pl.CostEstimate(flops=4_000_000_000, bytes_accessed=size * 2048 * n_out, transcendentals=0),
        name="merge",
    )(*arrays)


def final_kernel(chunks, s_ref, mix_ref, logits_ref, s0_ref, s1_ref, s2_ref, s3_ref, keep_ref, mate_ref, *refs):
    y_refs, far_refs, out_ref = refs[:chunks], refs[chunks:2 * chunks], refs[2 * chunks]
    mix = mix_ref[0]
    end = (s_ref[0] == 0) | (s_ref[0] == 3)
    size = PIECE // chunks
    metas = [r[size:size + META, :] for r in (keep_ref, mate_ref, y_refs[0], far_refs[0])]
    tops = [t[1:2] for t in metas]
    tops[3] = jnp.where(end, tops[3], -jnp.inf)
    top = functools.reduce(jnp.maximum, tops)
    scales = [jnp.exp(t - top) for t in tops]
    z = sum(t[0:1] * f for t, f in zip(metas, scales))
    scales = [f * (mix / z) for f in scales]
    stats = [r[...] for r in (s0_ref, s1_ref, s2_ref, s3_ref)]
    lm_top = functools.reduce(jnp.maximum, [t[:, :1] for t in stats])
    total = sum(t[:, 64:65] * jnp.exp(t[:, :1] - lm_top) for t in stats)
    lm_scale = (1.0 - mix) / total

    def lm(at, count):
        return jnp.exp(logits_ref[:, at:at + count] - lm_top) * lm_scale

    for i in range(0, PIECE, LANES):
        c, at = i // size, i % size
        base = c * (size + META) + at
        parts = [keep_ref[base:base + LANES, :], mate_ref[base:base + LANES, :], y_refs[c][at:at + LANES, :], far_refs[c][at:at + LANES, :]]
        h = sum(p * f for p, f in zip(parts, scales))
        h = h.T
        out_ref[:, i:i + LANES] = jnp.log(h[:64] + lm(i, LANES))
        count = min(LANES, UPPER - i)
        if count > 0:
            out_ref[:, PIECE + i:PIECE + i + count] = jnp.log(h[64:, :count] + lm(PIECE + i, count))


def final_call(s1, mix, logits, stats, keep, mate, from_y, far):
    vmem = pl.BlockSpec(memory_space=pltpu.VMEM)
    smem = pl.BlockSpec(memory_space=pltpu.SMEM)
    return pl.pallas_call(
        functools.partial(final_kernel, len(far)),
        in_specs=[smem, smem] + [vmem] * (7 + 2 * len(far)),
        out_specs=vmem,
        out_shape=jax.ShapeDtypeStruct(logits.shape, jnp.float32),
        compiler_params=pltpu.CompilerParams(vmem_limit_bytes=40 * 1024 * 1024),
        cost_estimate=pl.CostEstimate(flops=5_000_000_000, bytes_accessed=12 << 20, transcendentals=1 << 20),
        name="final",
    )(s1, mix, logits, *stats, keep, mate, *from_y, *far)


NEAR = [(0, 1), (1, 0), (2, 3), (3, 2)]
FAR2 = [(0, 2), (3, 1)]
FAR1 = [(1, 2), (2, 1)]
INWARD = [(0, 1), (3, 2)]
ACROSS = [(1, 3), (2, 0)]
CHUNKS = 2


def solution(mesh):
    store_devs = mesh.shape["store"]

    def swap(x, axis, bit):
        return lax.ppermute(x, axis, [(i, i ^ bit) for i in range(4)])

    def local_step(queries, w_head, store_keys, store_tok, temperature, mix_weight):
        rows_loc = queries.shape[0] // store_devs
        s = lax.axis_index("store")
        m = lax.axis_index("model")
        s1, m1 = s.reshape(1), m.reshape(1)
        tau = temperature.reshape(1)
        blocks = store_keys.shape[0] // BLOCK
        n_a = FIRST * BLOCK
        size = PIECE // CHUNKS
        tok2 = store_tok.reshape(-1, LANES)

        toks = [lax.ppermute(tok2, "store", NEAR), lax.ppermute(tok2, "store", FAR2), lax.ppermute(tok2, "store", FAR1)]
        rows_a = n_a // 2
        rows_b = store_keys.shape[0] // 2 - rows_a
        own, near_a, sparse_a, dense, code_own = score_call(s1, m1, tau, queries, store_keys, tok2, 0, FIRST, [])
        far2_a = lax.ppermute(sparse_a, "store", FAR2)
        far1_a = lax.ppermute(sparse_a, "store", FAR1)
        near_a = lax.ppermute(near_a, "store", NEAR)
        own, near_b, sparse_b, dense = score_call(s1, m1, tau, queries, store_keys, tok2, FIRST, blocks - FIRST, [own, dense])
        far2_b = lax.ppermute(sparse_b, "store", FAR2)
        far1_b = lax.ppermute(sparse_b, "store", FAR1)
        near_b = lax.ppermute(near_b, "store", NEAR)
        code_own = code_own.reshape(-1)
        codes = ids_call([near_a, far2_a, far1_a]).reshape(-1)
        n_all = n_a + 2 * rows_b

        dense = scatter_call(s1, [code_own], [dense], ((rows_a + rows_b, 0, 0, False),), None)
        d_next = swap(dense[3], "model", 1)
        d_mate = swap(dense[1], "model", 1)
        parts = merge_call(size, [dense[2], d_next], [(c, c) for c in range(CHUNKS)])
        d_y = [swap(parts[c], "model", 2) for c in range(CHUNKS)]

        segments = ((rows_a + rows_b, 0, 0, False), (rows_a, 1, 0, False), (rows_a, 1, n_all, True), (rows_a, 1, 2 * n_all, True))
        part = scatter_call(s1, [code_own, codes], [own, near_a, far2_a, far1_a], segments, None)
        segments = ((rows_b, 0, n_a, False), (rows_b, 0, n_all + n_a, True), (rows_b, 0, 2 * n_all + n_a, True))
        keep, mate, ynext, matey = scatter_call(s1, [codes], [near_b, far2_b, far1_b], segments, part)
        matey = swap(matey, "model", 1)
        mate = swap(mate, "model", 1)

        far = []
        for c in range(CHUNKS):
            plane, = merge_call(size, [dense[0], d_mate, d_y[c]], [(c, c, 0)])
            inward = lax.ppermute(plane, "store", INWARD)
            pair, = merge_call(size, [plane, inward], [(0, 0)])
            far.append(lax.ppermute(pair, "store", ACROSS))

        from_y = []
        for c in range(CHUNKS):
            part, = merge_call(size, [ynext, matey], [(c, c)])
            from_y.append(swap(part, "model", 2))

        my_rows = lax.dynamic_slice_in_dim(queries, s * rows_loc, rows_loc, axis=0)
        logits = lax.dot_general(my_rows, w_head, (((1,), (0,)), ((), ())), preferred_element_type=jnp.float32)
        lm_top = jnp.max(logits, axis=1, keepdims=True)
        lm_sum = jnp.sum(jnp.exp(logits - lm_top), axis=1, keepdims=True)
        stats = jnp.concatenate([jnp.broadcast_to(lm_top, (rows_loc, 64)), jnp.broadcast_to(lm_sum, (rows_loc, 64))], axis=1)
        stats = [stats] + [swap(stats, "model", k) for k in (1, 2, 3)]
        return final_call(s1, mix_weight.reshape(1), logits, stats, keep, mate, from_y, far)

    return jax.shard_map(local_step, mesh=mesh, in_specs=(P("data", None), P(None, "model"), P(("store", "model"), None), P(("store", "model")), P(), P()), out_specs=P(("data", "store"), "model"), check_vma=False)
```

```python
import functools

import jax
import jax.numpy as jnp
from jax import lax
from jax.experimental import pallas as pl
from jax.experimental.pallas import tpu as pltpu
from jax.sharding import PartitionSpec as P


LANES = 128
BLOCK = 512
BATCH = 16
WIDE = 2
VOCAB_LOC = 8000
PIECE = 4096
FIRST = 8
META = 8
SLOTS = 4
OUT_GROUP = 2
TOK_ROWS = 64
MERGE_STEPS = 4
VMEM = 66_900_000
STEP = 976
UPPER = VOCAB_LOC - PIECE
FLAG = 1 << 16
CLASH = 1 << 17


def targets(me):
    left = me < 2
    return me, me ^ 1, jnp.where(left, 2, 1), jnp.where(left, 3, 0)


def codes_of(tok, me):
    owner = sum((tok >= VOCAB_LOC * i).astype(jnp.int32) for i in (1, 2, 3))
    code = tok - owner * VOCAB_LOC + (owner ^ me) * VOCAB_LOC
    lane = lax.broadcasted_iota(jnp.int32, code.shape, 1)
    place = lane % BATCH
    clash = jnp.zeros_like(code)
    for d in range(1, BATCH):
        same = (code == pltpu.roll(code, LANES - d, 1)) & (place < BATCH - d)
        clash = clash | same.astype(jnp.int32)
    d = BATCH // 2
    while d:
        clash = clash | pltpu.roll(clash, LANES - d, 1)
        d //= 2
    first = place == 0
    group = jnp.max(jnp.where(first, clash, 0), axis=1, keepdims=True)
    marks = FLAG + jnp.where(clash > 0, CLASH, 0)
    return code + jnp.where(first & (group > 0), marks, 0)


def scores_kernel(first, count, carried, s_ref, m_ref, tau_ref, q_hbm, k_hbm, tok_ref, *refs):
    refs = refs[2:] if carried else refs
    outs, refs = refs[:4], refs[4:]
    if not carried:
        code_hbm, refs = refs[0], refs[1:]
    q_ref, qs_ref, held, stage, code_i, code_f, sem, q_sem, out_sem, tok_sem = refs
    half = BLOCK // 2
    group = OUT_GROUP * half

    def fetch(block):
        slot = lax.rem(block, SLOTS)
        rows = pl.ds(pl.multiple_of((first + block) * BLOCK, BLOCK), BLOCK)
        return pltpu.make_async_copy(k_hbm.at[rows], held.at[slot], sem.at[slot])

    def save(g):
        copies = []
        for i, out in enumerate(outs):
            start = g * group + (0 if i in (1, 2) else first * half)
            rows = pl.ds(pl.multiple_of(start, half), group)
            copies.append(pltpu.make_async_copy(stage.at[i, pl.ds(pl.multiple_of(g * group, half), group)], out.at[rows], out_sem.at[i, g]))
        return copies

    load_q = pltpu.make_async_copy(q_hbm, q_ref, q_sem)
    load_q.start()
    fetch(0).start()
    tokens = []
    if not carried:
        code_i[...] = codes_of(tok_ref[...], m_ref[0])
        code_f[...] = code_i[...].astype(jnp.float32)
        at = {1: outs[1].shape[0] - TOK_ROWS, 2: outs[2].shape[0] - TOK_ROWS}
        tokens = [pltpu.make_async_copy(code_f, outs[i].at[pl.ds(at[i], TOK_ROWS)], tok_sem.at[i - 1]) for i in (1, 2)]
        tokens.append(pltpu.make_async_copy(code_i, code_hbm, tok_sem.at[2]))
        for copy in tokens:
            copy.start()
    load_q.wait()
    for block in range(1, SLOTS - 1):
        fetch(block).start()
    for k, z in enumerate(targets(s_ref[0])):
        qs_ref[64 * k:64 * k + 64, :] = q_ref[pl.ds(pl.multiple_of(z * 64, 64), 64), :]
    low = lax.broadcasted_iota(jnp.int32, (half, LANES), 1) < 64

    @pl.loop(0, count)
    def _(block):
        @pl.when(block + SLOTS - 1 < count)
        def _():
            fetch(block + SLOTS - 1).start()

        fetch(block).wait()
        keys = held[lax.rem(block, SLOTS)]
        dots = lax.dot_general(keys, qs_ref[...], (((1,), (1,)), ((), ())), preferred_element_type=jnp.float32)
        wide = keys.astype(jnp.float32)
        norms = jnp.sum(wide * wide, axis=1, keepdims=True)
        scores = (2.0 * dots - norms) / tau_ref[0]
        out = pl.ds(pl.multiple_of(block * half, half), half)
        for k in range(4):
            tile = scores[:, LANES * (k // 2):LANES * (k // 2) + LANES]
            top, bottom = tile[:half], tile[half:]
            if k % 2 == 0:
                stage[k, out, :] = jnp.where(low, top, pltpu.roll(bottom, 64, 1))
            else:
                stage[k, out, :] = jnp.where(low, pltpu.roll(top, 64, 1), bottom)

        @pl.when(lax.rem(block, OUT_GROUP) == OUT_GROUP - 1)
        def _():
            for copy in save(block // OUT_GROUP):
                copy.start()

    for g in range(count // OUT_GROUP):
        for copy in save(g):
            copy.wait()
    for copy in tokens:
        copy.wait()


def score_call(me, model, tau, queries, keys, tok2, first, count, prev):
    width = keys.shape[1]
    whole = keys.shape[0] // 2
    rows = count * BLOCK // 2
    smem = pl.BlockSpec(memory_space=pltpu.SMEM)
    hbm = pl.BlockSpec(memory_space=pltpu.HBM)
    sent = (rows + (0 if prev else TOK_ROWS), LANES)
    shapes = [(whole, LANES), sent, sent, (whole, LANES)]
    return pl.pallas_call(
        functools.partial(scores_kernel, first, count, bool(prev)),
        in_specs=[smem, smem, smem, hbm, hbm, pl.BlockSpec(memory_space=pltpu.VMEM)] + [hbm] * len(prev),
        out_specs=[hbm] * (4 if prev else 5),
        out_shape=[jax.ShapeDtypeStruct(shape, jnp.float32) for shape in shapes] + ([] if prev else [jax.ShapeDtypeStruct(tok2.shape, jnp.int32)]),
        scratch_shapes=[
            pltpu.VMEM(queries.shape, queries.dtype),
            pltpu.VMEM(queries.shape, queries.dtype),
            pltpu.VMEM((SLOTS, BLOCK, width), keys.dtype),
            pltpu.VMEM((4, rows, LANES), jnp.float32),
            pltpu.VMEM((TOK_ROWS, LANES), jnp.int32),
            pltpu.VMEM((TOK_ROWS, LANES), jnp.float32),
            pltpu.SemaphoreType.DMA((SLOTS,)),
            pltpu.SemaphoreType.DMA,
            pltpu.SemaphoreType.DMA((4, count // OUT_GROUP)),
            pltpu.SemaphoreType.DMA((3,)),
        ],
        input_output_aliases={6: 0, 7: 3} if prev else {},
        compiler_params=pltpu.CompilerParams(vmem_limit_bytes=VMEM),
        cost_estimate=pl.CostEstimate(flops=2 * count * BLOCK * width * 256, bytes_accessed=count * BLOCK * width * 2, transcendentals=0),
        name="scores",
    )(me, model, tau, queries, keys, tok2, *prev)


def ids_kernel(*refs):
    n = len(refs) - 5
    srcs, (out_hbm, raw, ids, sem, out_sem) = refs[:n], refs[n:]
    loads = [pltpu.make_async_copy(r.at[pl.ds(r.shape[0] - TOK_ROWS, TOK_ROWS)], raw.at[i], sem.at[i]) for i, r in enumerate(srcs)]
    saves = [pltpu.make_async_copy(ids.at[i], out_hbm.at[pl.ds(i * TOK_ROWS, TOK_ROWS)], out_sem.at[i]) for i in range(n)]
    for load in loads:
        load.start()
    for i in range(n):
        loads[i].wait()
        ids[i] = raw[i].astype(jnp.int32)
        saves[i].start()
    for save in saves:
        save.wait()


def ids_call(arrays):
    n = len(arrays)
    hbm = pl.BlockSpec(memory_space=pltpu.HBM)
    shape = (n, TOK_ROWS, LANES)
    return pl.pallas_call(
        ids_kernel,
        in_specs=[hbm] * n,
        out_specs=hbm,
        out_shape=jax.ShapeDtypeStruct((n * TOK_ROWS, LANES), jnp.int32),
        scratch_shapes=[pltpu.VMEM(shape, jnp.float32), pltpu.VMEM(shape, jnp.int32), pltpu.SemaphoreType.DMA((n,)), pltpu.SemaphoreType.DMA((n,))],
        compiler_params=pltpu.CompilerParams(vmem_limit_bytes=VMEM),
        cost_estimate=pl.CostEstimate(flops=1_000_000, bytes_accessed=1 << 18, transcendentals=0),
        name="ids",
    )(*arrays)


def fold(row, op):
    wide = jnp.broadcast_to(row, (8, LANES))
    return op(wide, pltpu.roll(wide, 64, 1))[:1]


def scatter_kernel(segments, n_codes, chunks, carried, s_ref, *refs):
    n_x = len(segments)
    code_hbms, refs = refs[:n_codes], refs[n_codes:]
    x_hbms, refs = refs[:n_x], refs[n_x:]
    if carried:
        prev_hbms, refs = refs[:4], refs[4:]
    piece_hbms, refs = refs[:4], refs[4:]
    hist, e_ref, z_ref, stage, sem, prev_sem, out_sem = refs[:7]
    x_refs, refs = refs[7:7 + n_x], refs[7 + n_x:]
    code_refs, refs = refs[:n_codes], refs[n_codes:]
    piece_refs = [stage.at[rel] for rel in range(4)]
    half = BLOCK // 2
    loads = [pltpu.make_async_copy(a.at[pl.ds(0, b.shape[0])], b, sem.at[i]) for i, (a, b) in enumerate(zip(x_hbms, x_refs))]
    loads += [pltpu.make_async_copy(a, b, sem.at[n_x + i]) for i, (a, b) in enumerate(zip(code_hbms, code_refs))]
    for load in loads:
        load.start()
    if carried:
        prev, = refs
        prev_refs = [prev.at[rel] for rel in range(4)]
        prev_loads = [pltpu.make_async_copy(a, prev.at[i], prev_sem.at[i]) for i, a in enumerate(prev_hbms)]
        for load in prev_loads:
            load.start()
    saves = [pltpu.make_async_copy(stage.at[rel], piece_hbms[rel], out_sem.at[rel]) for rel in range(4)]

    @pl.loop(0, hist.shape[0] // 320)
    def _(i):
        hist[pl.ds(pl.multiple_of(i * 320, 320), 320), :] = jnp.zeros((320, LANES), jnp.float32)

    z_ref[...] = jnp.zeros_like(z_ref)
    for load in loads:
        load.wait()
    middle = (s_ref[0] == 1) | (s_ref[0] == 2)
    counts = [jnp.where(middle, x.shape[0] // (WIDE * half), 0) if seg[2] else x.shape[0] // (WIDE * half) for x, seg in zip(x_refs, segments)]
    peak = jnp.full((8, LANES), -jnp.inf, jnp.float32)
    for x_ref, count in zip(x_refs, counts):
        def widen(block, peak):
            x = x_ref[pl.ds(pl.multiple_of(block * WIDE * half, WIDE * half), WIDE * half), :]
            return jnp.maximum(peak, jnp.max(x.reshape(WIDE * half // 8, 8, LANES), axis=0))

        peak = lax.fori_loop(0, count, widen, peak)
    top = fold(jnp.max(peak, axis=0, keepdims=True), jnp.maximum)

    for x_ref, (which, base, _), count in zip(x_refs, segments, counts):
        code_ref = code_refs[which]

        @pl.loop(0, count)
        def _(block):
            wide = pl.ds(pl.multiple_of(block * WIDE * half, WIDE * half), WIDE * half)
            e = jnp.exp(x_ref[wide, :] - top)
            z_ref[...] += jnp.sum(e.reshape(WIDE * half // 8, 8, LANES), axis=0)
            for i in range(WIDE):
                part = e[i * half:i * half + half]
                e_ref[i * BLOCK:i * BLOCK + half] = part
                e_ref[i * BLOCK + half:i * BLOCK + BLOCK] = pltpu.roll(part, 64, 1)

            @pl.loop(0, WIDE * BLOCK // LANES)
            def _(group):
                row = pl.multiple_of(group * LANES, LANES)
                at = pl.multiple_of(base + block * WIDE * BLOCK + group * LANES, LANES)
                rows_ref = e_ref.at[pl.ds(row, LANES)]
                head = code_ref[at]

                @pl.when(head < FLAG)
                def _():
                    for b in range(0, LANES, BATCH):
                        ids = [code_ref.at[pl.ds(b + i, code_ref.shape[0] - LANES + 1)][at] for i in range(BATCH)]
                        new = [hist[pl.ds(ids[i], 1), :] + rows_ref[b + i:b + i + 1, :] for i in range(BATCH)]
                        for i in range(BATCH):
                            hist[pl.ds(ids[i], 1), :] = new[i]

                @pl.when(head >= FLAG)
                def _():
                    @pl.loop(0, LANES // BATCH)
                    def _(b):
                        mark = code_ref[at + b * BATCH]
                        ids = [mark & (FLAG - 1)] + [code_ref[at + b * BATCH + i] for i in range(1, BATCH)]
                        rows = rows_ref.at[pl.ds(pl.multiple_of(b * BATCH, BATCH), BATCH)]

                        @pl.when((mark & CLASH) == 0)
                        def _():
                            new = [hist[pl.ds(ids[i], 1), :] + rows[i:i + 1, :] for i in range(BATCH)]
                            for i in range(BATCH):
                                hist[pl.ds(ids[i], 1), :] = new[i]

                        @pl.when((mark & CLASH) != 0)
                        def _():
                            for i in range(BATCH):
                                hist[pl.ds(ids[i], 1), :] += rows[i:i + 1, :]

    size = PIECE // chunks
    z = fold(jnp.sum(z_ref[...], axis=0, keepdims=True), jnp.add)
    scale = held_scale = None
    if carried:
        for load in prev_loads:
            load.wait()
        held_top = prev_refs[0][size + 1:size + 2, :]
        both = jnp.maximum(top, held_top)
        scale, held_scale = jnp.exp(top - both), jnp.exp(held_top - both)
        z = z * scale + prev_refs[0][size:size + 1, :] * held_scale
        top = both
    meta = jnp.concatenate([z, top, jnp.zeros((META - 2, LANES), jnp.float32)], axis=0)

    def place(rel, c, at, rows, both):
        first = c * size + at
        lower = hist[pl.ds(pl.multiple_of(rel * VOCAB_LOC + first, 8), rows), :]
        low = lax.broadcasted_iota(jnp.int32, (rows, LANES), 1) < 64
        if both:
            value = jnp.where(low, lower, pltpu.roll(hist[pl.ds(pl.multiple_of(rel * VOCAB_LOC + PIECE + first, 8), rows), :], 64, 1))
        else:
            value = jnp.where(low, lower, 0.0)
        if carried:
            value = value * scale + prev_refs[rel][pl.ds(pl.multiple_of(first + c * META, 8), rows), :] * held_scale
        piece_refs[rel][pl.ds(pl.multiple_of(c * (size + META) + at, 8), rows), :] = value

    for rel in (3, 1, 2, 0):
        for c in range(chunks):
            full = min(size, UPPER - c * size)

            @pl.loop(0, full // STEP)
            def _(i):
                place(rel, c, i * STEP, STEP, True)

            rest = full % STEP
            if rest:
                place(rel, c, full - rest, rest, True)
            if full < size:
                place(rel, c, full, size - full, False)
            at = c * (size + META) + size
            piece_refs[rel][at:at + META, :] = meta
        saves[rel].start()
    for save in saves:
        save.wait()


def scatter_call(s1, codes, xs, segments, prev):
    n_codes = len(codes)
    carried = prev is not None
    smem = pl.BlockSpec(memory_space=pltpu.SMEM)
    hbm = pl.BlockSpec(memory_space=pltpu.HBM)
    piece = jax.ShapeDtypeStruct((PIECE + CHUNKS * META, LANES), jnp.float32)
    n_keys = sum(2 * seg[0] for seg in segments)
    whole = pltpu.VMEM((4, *piece.shape), jnp.float32)
    return pl.pallas_call(
        functools.partial(scatter_kernel, tuple(seg[1:] for seg in segments), n_codes, CHUNKS, carried),
        in_specs=[smem] + [hbm] * (n_codes + len(xs) + (4 if carried else 0)),
        out_specs=[hbm] * 4,
        out_shape=[piece] * 4,
        scratch_shapes=[
            pltpu.VMEM((4 * VOCAB_LOC, LANES), jnp.float32),
            pltpu.VMEM((WIDE * BLOCK, LANES), jnp.float32),
            pltpu.VMEM((8, LANES), jnp.float32),
            whole,
            pltpu.SemaphoreType.DMA((len(xs) + n_codes,)),
            pltpu.SemaphoreType.DMA((4,)),
            pltpu.SemaphoreType.DMA((4,)),
        ]
        + [pltpu.VMEM((seg[0], LANES), jnp.float32) for seg in segments]
        + [pltpu.SMEM(c.shape, jnp.int32) for c in codes]
        + ([whole] if carried else []),
        compiler_params=pltpu.CompilerParams(vmem_limit_bytes=VMEM),
        cost_estimate=pl.CostEstimate(flops=n_keys * 1_000_000, bytes_accessed=n_keys * 512, transcendentals=n_keys * 64),
        name="scatter",
    )(s1, *codes, *xs, *(prev if carried else ()))


def merge_kernel(size, groups, *refs):
    n, n_out = len(groups[0]), len(groups)
    srcs, outs, refs = refs[:n], refs[n:n + n_out], refs[n + n_out:]
    stages, sem, out_sem, bufs = refs[:n_out], refs[n_out], refs[n_out + 1], refs[n_out + 2:]
    step = size // MERGE_STEPS
    parts = [(size, META)] + [(i * step, step) for i in range(MERGE_STEPS)]
    work = []
    for g, offsets in enumerate(groups):
        mine = bufs[g * n:g * n + n]
        loads = [[pltpu.make_async_copy(r.at[pl.ds(o + at, rows)], b.at[pl.ds(at, rows)], sem.at[g, i, j]) for i, (r, o, b) in enumerate(zip(srcs, offsets, mine))] for j, (at, rows) in enumerate(parts)]
        saves = [pltpu.make_async_copy(stages[g].at[pl.ds(at, rows)], outs[g].at[pl.ds(at, rows)], out_sem.at[g, j]) for j, (at, rows) in enumerate(parts)]
        work.append((mine, loads, saves, stages[g]))
    for _, loads, _, _ in work:
        for group in loads:
            for load in group:
                load.start()
    for mine, loads, saves, stage in work:
        for j, (at, rows) in enumerate(parts):
            for load in loads[j]:
                load.wait()
            if j == 0:
                tops = [b[size + 1:size + 2, :] for b in mine]
                top = functools.reduce(jnp.maximum, tops)
                scales = [jnp.exp(t - top) for t in tops]
            total = functools.reduce(jnp.add, [b[at:at + rows, :] * f for b, f in zip(mine, scales)])
            if j == 0:
                total = jnp.where(lax.broadcasted_iota(jnp.int32, (META, LANES), 0) == 1, top, total)
            stage[at:at + rows, :] = total
            saves[j].start()
    for _, _, saves, _ in work:
        for save in saves:
            save.wait()


def merge_call(size, arrays, groups):
    hbm = pl.BlockSpec(memory_space=pltpu.HBM)
    shape = (size + META, LANES)
    n, n_out = len(arrays), len(groups)
    return pl.pallas_call(
        functools.partial(merge_kernel, size, tuple(tuple(c * (size + META) for c in group) for group in groups)),
        in_specs=[hbm] * n,
        out_specs=[hbm] * n_out,
        out_shape=[jax.ShapeDtypeStruct(shape, jnp.float32)] * n_out,
        scratch_shapes=[pltpu.VMEM(shape, jnp.float32)] * n_out
        + [pltpu.SemaphoreType.DMA((n_out, n, MERGE_STEPS + 1)), pltpu.SemaphoreType.DMA((n_out, MERGE_STEPS + 1))]
        + [pltpu.VMEM(shape, jnp.float32)] * (n * n_out),
        compiler_params=pltpu.CompilerParams(vmem_limit_bytes=VMEM),
        cost_estimate=pl.CostEstimate(flops=4_000_000_000, bytes_accessed=size * 2048 * n_out, transcendentals=0),
        name="merge",
    )(*arrays)


def final_kernel(chunks, s_ref, mix_ref, logits_ref, s0_ref, s1_ref, s2_ref, s3_ref, *refs):
    home_refs, y_refs, far_refs, out_ref = refs[:chunks], refs[chunks:2 * chunks], refs[2 * chunks:3 * chunks], refs[3 * chunks]
    mix = mix_ref[0]
    end = (s_ref[0] == 0) | (s_ref[0] == 3)
    size = PIECE // chunks
    metas = [r[size:size + META, :] for r in (home_refs[0], y_refs[0], far_refs[0])]
    tops = [t[1:2] for t in metas]
    tops[2] = jnp.where(end, tops[2], -jnp.inf)
    top = functools.reduce(jnp.maximum, tops)
    scales = [jnp.exp(t - top) for t in tops]
    z = sum(t[0:1] * f for t, f in zip(metas, scales))
    scales = [f * (mix / z) for f in scales]
    stats = [r[...] for r in (s0_ref, s1_ref, s2_ref, s3_ref)]
    lm_top = functools.reduce(jnp.maximum, [t[:, :1] for t in stats])
    total = sum(t[:, 64:65] * jnp.exp(t[:, :1] - lm_top) for t in stats)
    lm_scale = (1.0 - mix) / total

    def lm(at, count):
        return jnp.exp(logits_ref[:, at:at + count] - lm_top) * lm_scale

    for i in range(0, PIECE, LANES):
        c, at = i // size, i % size
        parts = [r[c][at:at + LANES, :] for r in (home_refs, y_refs, far_refs)]
        h = sum(p * f for p, f in zip(parts, scales))
        h = h.T
        out_ref[:, i:i + LANES] = jnp.log(h[:64] + lm(i, LANES))
        count = min(LANES, UPPER - i)
        if count > 0:
            out_ref[:, PIECE + i:PIECE + i + count] = jnp.log(h[64:, :count] + lm(PIECE + i, count))


def final_call(s1, mix, logits, stats, home, from_y, far):
    vmem = pl.BlockSpec(memory_space=pltpu.VMEM)
    smem = pl.BlockSpec(memory_space=pltpu.SMEM)
    return pl.pallas_call(
        functools.partial(final_kernel, len(far)),
        in_specs=[smem, smem] + [vmem] * (5 + 3 * len(far)),
        out_specs=vmem,
        out_shape=jax.ShapeDtypeStruct(logits.shape, jnp.float32),
        compiler_params=pltpu.CompilerParams(vmem_limit_bytes=40 * 1024 * 1024),
        cost_estimate=pl.CostEstimate(flops=5_000_000_000, bytes_accessed=12 << 20, transcendentals=1 << 20),
        name="final",
    )(s1, mix, logits, *stats, *home, *from_y, *far)


NEAR = [(0, 1), (1, 0), (2, 3), (3, 2)]
FAR2 = [(0, 2), (3, 1)]
FAR1 = [(1, 2), (2, 1)]
INWARD = [(0, 1), (3, 2)]
ACROSS = [(1, 3), (2, 0)]
CHUNKS = 2


def solution(mesh):
    store_devs = mesh.shape["store"]

    def swap(x, axis, bit):
        return lax.ppermute(x, axis, [(i, i ^ bit) for i in range(4)])

    def local_step(queries, w_head, store_keys, store_tok, temperature, mix_weight):
        rows_loc = queries.shape[0] // store_devs
        s = lax.axis_index("store")
        m = lax.axis_index("model")
        s1, m1 = s.reshape(1), m.reshape(1)
        tau = temperature.reshape(1)
        blocks = store_keys.shape[0] // BLOCK
        n_a = FIRST * BLOCK
        size = PIECE // CHUNKS
        tok2 = store_tok.reshape(-1, LANES)

        toks = [lax.ppermute(tok2, "store", NEAR), lax.ppermute(tok2, "store", FAR2), lax.ppermute(tok2, "store", FAR1)]
        rows_a = n_a // 2
        rows_b = store_keys.shape[0] // 2 - rows_a
        own, near_a, sparse_a, dense, code_own = score_call(s1, m1, tau, queries, store_keys, tok2, 0, FIRST, [])
        far2_a = lax.ppermute(sparse_a, "store", FAR2)
        far1_a = lax.ppermute(sparse_a, "store", FAR1)
        near_a = lax.ppermute(near_a, "store", NEAR)
        own, near_b, sparse_b, dense = score_call(s1, m1, tau, queries, store_keys, tok2, FIRST, blocks - FIRST, [own, dense])
        far2_b = lax.ppermute(sparse_b, "store", FAR2)
        far1_b = lax.ppermute(sparse_b, "store", FAR1)
        near_b = lax.ppermute(near_b, "store", NEAR)
        code_own = code_own.reshape(-1)
        codes = ids_call([near_a, far2_a, far1_a]).reshape(-1)
        n_all = n_a + 2 * rows_b

        dense = scatter_call(s1, [code_own], [dense], ((rows_a + rows_b, 0, 0, False),), None)
        d_next = swap(dense[3], "model", 1)
        d_mate = swap(dense[1], "model", 1)
        parts = merge_call(size, [dense[2], d_next], [(c, c) for c in range(CHUNKS)])
        d_y = [swap(parts[c], "model", 2) for c in range(CHUNKS)]

        segments = ((rows_a + rows_b, 0, 0, False), (rows_a, 1, 0, False), (rows_a, 1, n_all, True), (rows_a, 1, 2 * n_all, True))
        part = scatter_call(s1, [code_own, codes], [own, near_a, far2_a, far1_a], segments, None)
        segments = ((rows_b, 0, n_a, False), (rows_b, 0, n_all + n_a, True), (rows_b, 0, 2 * n_all + n_a, True))
        keep, mate, ynext, matey = scatter_call(s1, [codes], [near_b, far2_b, far1_b], segments, part)
        matey = swap(matey, "model", 1)
        mate = swap(mate, "model", 1)

        far = []
        for c in range(CHUNKS):
            plane, = merge_call(size, [dense[0], d_mate, d_y[c]], [(c, c, 0)])
            inward = lax.ppermute(plane, "store", INWARD)
            pair, = merge_call(size, [plane, inward], [(0, 0)])
            far.append(lax.ppermute(pair, "store", ACROSS))

        from_y = []
        for c in range(CHUNKS):
            part, = merge_call(size, [ynext, matey], [(c, c)])
            from_y.append(swap(part, "model", 2))

        home = merge_call(size, [keep, mate], [(c, c) for c in range(CHUNKS)])
        my_rows = lax.dynamic_slice_in_dim(queries, s * rows_loc, rows_loc, axis=0)
        logits = lax.dot_general(my_rows, w_head, (((1,), (0,)), ((), ())), preferred_element_type=jnp.float32)
        lm_top = jnp.max(logits, axis=1, keepdims=True)
        lm_sum = jnp.sum(jnp.exp(logits - lm_top), axis=1, keepdims=True)
        stats = jnp.concatenate([jnp.broadcast_to(lm_top, (rows_loc, 64)), jnp.broadcast_to(lm_sum, (rows_loc, 64))], axis=1)
        stats = [stats] + [swap(stats, "model", k) for k in (1, 2, 3)]
        return final_call(s1, mix_weight.reshape(1), logits, stats, home, from_y, far)

    return jax.shard_map(local_step, mesh=mesh, in_specs=(P("data", None), P(None, "model"), P(("store", "model"), None), P(("store", "model")), P(), P()), out_specs=P(("data", "store"), "model"), check_vma=False)
```
